32 devices in a mesh: gx: 2 (over x), gy: 4 (over y, core), gz: 4 (over z).
Axes of the slice: x: 2, y: 2, z: 4, core: 2. Of those that a mesh axis runs over, the one named last changes fastest.
Arguments:
- right_side: float32 [4, 5, 2, 32, 512], P(None, None, 'gx', 'gy', 'gz'), may hold values from -6 to 6
- jacobian: bfloat16 [27, 5, 5, 2, 32, 512], P(None, None, None, 'gx', 'gy', 'gz'), may hold values from -0.14 to 12.14, as said below
Outputs:
- solution: float32 [4, 5, 2, 32, 512], P(None, None, 'gx', 'gy', 'gz')
- residual: float32 [4, 5, 2, 32, 512], P(None, None, 'gx', 'gy', 'gz')
The draws below stay inside these ranges and needn't reach their ends.
Inputs may be any that keep to these rules, and one draw needn't show every extreme that they name: `jacobian`: blocks of offsets other than 13 and the off-diagonal entries of block 13 lie within -0.14 to 0.14; the diagonal entries of block 13 exceed 5.8 in every cell.
All inputs are finite; a program needn't handle non-finite values.
Results may differ from the reference program's by a relative error of at most 0.0003.
Values sent between devices are 32-bit elements.
A program may use at most 64 MiB of HBM per device.

```python
import jax
import jax.numpy as jnp
from jax import lax

COMP = 5
RHS = 4
STENCIL = 27
ITERS = 3
NX = 2
NY = 32
NZ = 512


def draw_jacobian(key, part):
    first_key, second_key = jax.random.split(jax.random.fold_in(key, 17))
    full_shape = (STENCIL, COMP, COMP, NX, NY, NZ)
    diag_shape = (COMP, NX, NY, NZ)
    entries = jax.random.uniform(first_key, full_shape, jnp.float32, -0.14, 0.14)
    diagonal = jax.random.uniform(second_key, diag_shape, jnp.float32, 6.0, 12.0)
    identity = jnp.eye(COMP, dtype=jnp.float32)[:, :, None, None, None]
    center = entries[13] + identity * diagonal[:, None]
    entries = entries.at[13].set(center)
    return entries.astype(jnp.bfloat16)


def levels(rng, extent, shards, least, high):
    level = 1.0
    for axis_at, blocks in shards:
        heights = jax.random.uniform(jax.random.fold_in(jax.random.fold_in(rng, 6), axis_at), (blocks,), jnp.float32, least / len(shards), high / len(shards))
        level = level * jnp.repeat(jnp.exp(heights), extent[axis_at] // blocks).reshape((-1,) + (1,) * (len(extent) - 1 - axis_at))
    return level


def noise(rng, extent, deviation, bound, shards=(), kind=jnp.bfloat16):
    array = jax.random.normal(rng, extent, jnp.float32) * deviation
    if len(shards) > 0:
        array = levels(rng, extent, shards, -0.22, 0.18) * array
    return jnp.clip(array, min=-bound, max=bound).astype(kind)


def setup_inputs(seed: int = 0) -> dict:
    streams_of = jax.random.split(jax.random.key(seed), 3)
    return {
        "right_side": noise(streams_of[0], (RHS, COMP, NX, NY, NZ), 1.0, 6.0, ((2, 2), (3, 4), (4, 4)), jnp.float32),
        "jacobian": draw_jacobian(jax.random.fold_in(streams_of[2], 71), 0),
    }


def dot_high(left, right):
    return jnp.dot(left.astype(jnp.float32), right.astype(jnp.float32), precision=lax.Precision.HIGHEST, preferred_element_type=jnp.float32)

def lower_solve(factor, target):
    solved = []
    for row_pos in range(factor.shape[0]):
        accum = target[row_pos]
        for prior in range(row_pos):
            accum = accum - factor[row_pos, prior] * solved[prior]
        solved.append(accum / factor[row_pos, row_pos])
    return jnp.stack(solved)

def upper_solve(factor, target):
    size_all = factor.shape[0]
    solved = [None] * size_all
    for row_pos in range(size_all - 1, -1, -1):
        accum = target[row_pos]
        for later in range(row_pos + 1, size_all):
            accum = accum - factor[later, row_pos] * solved[later]
        solved[row_pos] = accum / factor[row_pos, row_pos]
    return jnp.stack(solved)

def extend(field):
    padded = jnp.pad(field, ((0, 0), (0, 0), (1, 1), (1, 1), (0, 0)), mode='wrap')
    return jnp.pad(padded, ((0, 0), (0, 0), (0, 0), (0, 0), (1, 1)))

def apply_operator(jacobian, padded):
    extent_x = padded.shape[2] - 2
    extent_y = padded.shape[3] - 2
    extent_z = padded.shape[4] - 2
    total = jnp.zeros((padded.shape[0], padded.shape[1], extent_x, extent_y, extent_z), jnp.float32)
    for stencil_pos in range(27):
        start_x = stencil_pos // 9
        start_y = stencil_pos // 3 % 3
        start_z = stencil_pos % 3
        piece = padded[:, :, start_x:start_x + extent_x, start_y:start_y + extent_y, start_z:start_z + extent_z]
        block = jacobian[stencil_pos].astype(jnp.float32)
        for source_comp in range(block.shape[1]):
            total = total + block[None, :, source_comp] * piece[:, source_comp][:, None]
    return total

def reference(right_side, jacobian):
    field_shape = right_side.shape
    rhs_count = field_shape[0]
    flat_rhs = right_side.reshape(rhs_count, -1)
    start_factor = jnp.linalg.cholesky(dot_high(flat_rhs, flat_rhs.T))
    basis = [lower_solve(start_factor, flat_rhs)]
    hessen_rows = []
    for iteration in range(ITERS):
        workspace = apply_operator(jacobian, extend(basis[-1].reshape(field_shape))).reshape(rhs_count, -1)
        stacked = jnp.concatenate(basis, axis=0)
        coefficients = dot_high(stacked, workspace.T)
        workspace = workspace - dot_high(coefficients.T, stacked)
        factor = jnp.linalg.cholesky(dot_high(workspace, workspace.T))
        basis.append(lower_solve(factor, workspace))
        filler = jnp.zeros((rhs_count, rhs_count * (ITERS - iteration - 1)), jnp.float32)
        hessen_rows.append(jnp.concatenate([coefficients.T, factor, filler], axis=1))
    hessen = jnp.concatenate(hessen_rows, axis=0)
    target = jnp.concatenate([start_factor, jnp.zeros((rhs_count, rhs_count * ITERS), jnp.float32)], axis=1)
    normal_factor = jnp.linalg.cholesky(dot_high(hessen, hessen.T))
    middle = lower_solve(normal_factor, dot_high(hessen, target.T))
    weights = upper_solve(normal_factor, middle)
    solution = dot_high(weights.T, jnp.concatenate(basis[:-1], axis=0))
    solution_field = solution.reshape(field_shape)
    residual = right_side - apply_operator(jacobian, extend(solution_field))
    return (solution_field, residual)
```

```python
import functools
import itertools

import jax
import jax.numpy as jnp
from jax import lax
from jax.experimental import pallas as pl
from jax.experimental.pallas import tpu as pltpu
from jax.sharding import PartitionSpec as P

ITERS = 3
SHIFT = 9.0
MESH = pl.DeviceIdType.MESH
AXES = ("gx", "gy", "gz")


def make_kernel(sizes, rhs, comp, rows, lanes):
    count_x, count_y, count_z = sizes
    devices = count_x * count_y * count_z
    fields = rhs * comp
    merged = count_x == 2
    near_only = max(count_x // 2, count_y // 2, count_z - 1) <= ITERS
    plane_steps = (0, 1) if merged else (0, 1, -1)
    planes = len(plane_steps)
    slots = 9 + rhs
    pair_list = []
    vectors = rhs * (ITERS + 1)
    for step in range(1, ITERS + 1):
        for mine in range(rhs * step, rhs * (step + 1)):
            for other in range(0, mine + 1):
                pair_list.append((mine, other))
    pair_slot = {pair: slot for slot, pair in enumerate(pair_list)}
    pair_pad = -(-len(pair_list) // 128) * 128

    def kernel(
        right_hbm, jac_hbm, sol_ref, res_ref,
        right_ref, basis, prods, jac_low, jac, shifted, packs, edge_rows, edge_corner,
        far_plane, halo_rows, halo_cols, halo_corner, tops, gram, part, parts,
        right_sem, jac_sem, send_sem, recv_sem, red_send, red_recv,
    ):
        my_x, my_y, my_z = (lax.axis_index(axis) for axis in AXES)
        me = (my_x * count_y + my_y) * count_z + my_z

        def coords(index):
            return (index // (count_y * count_z), index // count_z % count_y, index % count_z)

        def beside(step_x, dy, dz):
            return (
                lax.rem(my_x + step_x + count_x, count_x),
                lax.rem(my_y + dy + count_y, count_y),
                jnp.clip(my_z + dz, 0, count_z - 1),
            )

        above = my_z < count_z - 1
        below = my_z > 0
        barrier = pltpu.get_barrier_semaphore()

        def salute(device):
            pl.semaphore_signal(barrier, inc=1, device_id=device, device_id_type=MESH)

        if near_only:
            for dz in (1, -1, 0):
                offsets = [
                    (step_x, dy)
                    for step_x, dy in itertools.product(reversed(plane_steps), (1, -1, 0))
                    if (step_x, dy, dz) != (0, 0, 0)
                ]

                def greet_layer():
                    for step_x, dy in offsets:
                        salute(beside(step_x, dy, dz))

                if dz == 0:
                    greet_layer()
                else:
                    pl.when(above if dz == 1 else below)(greet_layer)
            greeted = planes * 3 * (1 + above.astype(jnp.int32) + below.astype(jnp.int32)) - 1
        else:

            def greet(step, carry):
                salute(coords(lax.rem(me + step, devices)))
                return carry

            lax.fori_loop(1, devices, greet, 0)
            greeted = devices - 1

        right_load = pltpu.make_async_copy(right_hbm, right_ref, right_sem)
        right_load.start()
        loads = pltpu.make_async_copy(jac_hbm, jac_low, jac_sem)
        loads.start()

        lane = lax.broadcasted_iota(jnp.int32, (rows, lanes), 1)
        sub = lax.broadcasted_iota(jnp.int32, (rows, lanes), 0)

        def field(turn, at):
            return right_ref[at] if turn == 0 else basis[turn - 1, at]

        def pack(turn):
            packed = jnp.zeros((rows, lanes), jnp.float32)
            for at in range(fields):
                value = field(turn, at)
                edge_rows[turn, 0, at : at + 1, :] = value[rows - 1 : rows]
                edge_rows[turn, 1, at : at + 1, :] = value[0:1]
                packed = jnp.where(lane // 2 == at, pltpu.roll(value, 2 * at + 1, 1), packed)
            packs[turn] = packed
            edge_corner[turn, 0] = packed[rows - 1 : rows]
            edge_corner[turn, 1] = packed[0:1]

        def messages(turn):
            found = []
            for plane, step_x in enumerate(plane_steps):
                for dy, dz in itertools.product((1, -1, 0), (1, -1, 0)):
                    side_y = 0 if dy == 1 else 1
                    side_z = 0 if dz == 1 else 1
                    if dy == 0 and dz == 0:
                        if plane == 0:
                            continue
                        values = right_ref if turn == 0 else basis.at[turn - 1]
                        moves = [
                            (values.at[pl.ds(r * comp, comp)], far_plane.at[turn, plane - 1, pl.ds(r * comp, comp)])
                            for r in range(rhs)
                        ]
                    elif dz == 0:
                        moves = [(edge_rows.at[turn, side_y], halo_rows.at[turn, plane, side_y])]
                    elif dy == 0:
                        moves = [(packs.at[turn], halo_cols.at[turn, plane, side_z])]
                    else:
                        moves = [(edge_corner.at[turn, side_y], halo_corner.at[turn, plane, side_y, side_z])]
                    for part_at, (source, target) in enumerate(moves):
                        slot = plane * slots
                        if len(moves) == 1:
                            slot = slot + (dy + 1) * 3 + dz + 1
                        else:
                            slot = slot + 9 + part_at
                        copy = pltpu.make_async_remote_copy(
                            src_ref=source,
                            dst_ref=target,
                            send_sem=send_sem.at[turn, slot],
                            recv_sem=recv_sem.at[turn, slot],
                            device_id=beside(step_x, dy, dz),
                            device_id_type=MESH,
                        )
                        found.append((plane, dz, copy, part_at if len(moves) > 1 else None))
            return found

        def for_each(copies, act, sending):
            for step_z in (1, -1, 0):
                chosen = [copy for _, dz, copy, _ in copies if dz == step_z]
                if step_z == 0:
                    for copy in chosen:
                        act(copy)
                else:
                    present = above if (step_z == 1) == sending else below

                    @pl.when(present)
                    def _():
                        for copy in chosen:
                            act(copy)

        def shift_edges(turn, plane):
            low = jnp.where(below, pltpu.roll(halo_cols[turn, plane, 0], 1, 1), 0.0)
            high = jnp.where(above, pltpu.roll(halo_cols[turn, plane, 1], lanes - 1, 1), 0.0)
            mixed = jnp.where(lane % 2 == 1, low, high)
            wide_lane = lax.broadcasted_iota(jnp.int32, (fields, lanes), 1)
            wide_at = lax.broadcasted_iota(jnp.int32, (fields, lanes), 0)
            for side in range(2):
                strip = halo_rows[turn, plane, side]
                low_row = jnp.where(below, halo_corner[turn, plane, side, 0], 0.0)
                high_row = jnp.where(above, halo_corner[turn, plane, side, 1], 0.0)
                low_col = jnp.sum(
                    jnp.where(wide_lane == 2 * wide_at, low_row, 0.0), axis=1, keepdims=True
                )
                high_col = jnp.sum(
                    jnp.where(wide_lane == 2 * wide_at + 1, high_row, 0.0), axis=1, keepdims=True
                )
                tops[side, 0] = jnp.where(wide_lane == 0, low_col, pltpu.roll(strip, 1, 1))
                tops[side, 1] = strip
                tops[side, 2] = jnp.where(
                    wide_lane == lanes - 1, high_col, pltpu.roll(strip, lanes - 1, 1)
                )
            return mixed

        def shift_fields(turn, plane, mixed, first, last):
            for at in range(first, last):
                value = field(turn, at) if plane == 0 else far_plane[turn, plane - 1, at]
                edge = pltpu.roll(mixed, lanes - 2 * at - 1, 1)
                along = (
                    jnp.where(lane == 0, edge, pltpu.roll(value, 1, 1)),
                    value,
                    jnp.where(lane == lanes - 1, edge, pltpu.roll(value, lanes - 1, 1)),
                )
                for dz in range(3):
                    shifted[dz, at] = jnp.where(
                        sub == 0, tops[0, dz, at : at + 1, :], pltpu.roll(along[dz], 1, 0)
                    )
                    shifted[3 + dz, at] = along[dz]
                    shifted[6 + dz, at] = jnp.where(
                        sub == rows - 1,
                        tops[1, dz, at : at + 1, :],
                        pltpu.roll(along[dz], rows - 1, 0),
                    )

        def stencil(plane, totals, sides):
            def body(line, sums):
                sums = list(sums)
                for near, source in itertools.product(range(3), range(comp)):
                    near = line * 3 + near
                    blocks = [jac[plane, near, a * comp + source] for a in range(comp)]
                    for place, r in enumerate(sides):
                        value = shifted[near, r * comp + source]
                        for a in range(comp):
                            sums[place * comp + a] = sums[place * comp + a] + blocks[a] * value
                return tuple(sums)

            return list(lax.fori_loop(0, 3, body, tuple(totals)))

        def vector(index, c):
            if index < rhs:
                return right_ref[index * comp + c]
            return prods[index // rhs - 1, (index % rhs) * comp + c]

        def dots(step):
            for mine in range(rhs * step, rhs * (step + 1)):
                own = [vector(mine, c) for c in range(comp)]
                for other in range(0, mine + 1):
                    total = own[0] * vector(other, 0)
                    for c in range(1, comp):
                        total = total + own[c] * vector(other, c)
                    gram[pair_slot[mine, other]] = total

        for slot in range(len(pair_list), pair_pad):
            gram[slot] = jnp.zeros((rows, lanes), jnp.float32)
        right_load.wait()
        pack(0)
        pl.semaphore_wait(barrier, greeted)
        for_each(messages(0), lambda copy: copy.start(), True)
        loads.wait()

        def widen(near, carry):
            for entry in range(comp * comp):
                jac[0, near, entry] = jac_low[9 + near, entry].astype(jnp.float32)
                first = jac_low[near, entry].astype(jnp.float32)
                last = jac_low[18 + near, entry].astype(jnp.float32)
                if merged:
                    jac[1, near, entry] = first + last
                else:
                    jac[1, near, entry] = first
                    jac[2, near, entry] = last
            return carry

        lax.fori_loop(0, 9, widen, 0)

        for turn in range(ITERS):
            copies = messages(turn)
            if turn > 0:
                for_each(copies, lambda copy: copy.start(), True)
                dots(turn)
            totals = [jnp.zeros((rows, lanes), jnp.float32) for _ in range(fields)]
            for plane in range(planes):
                mine = [copy for copy in copies if copy[0] == plane and copy[3] is None]
                for_each(mine, lambda copy: copy.wait_recv(), False)
                mixed = shift_edges(turn, plane)
                if plane == 0:
                    shift_fields(turn, plane, mixed, 0, fields)
                    totals = stencil(plane, totals, range(rhs))
                    for at in range(fields):
                        prods[turn, at] = totals[at]
                    continue
                for r in range(rhs):
                    for copy in copies:
                        if copy[0] == plane and copy[3] == r:
                            copy[2].wait_recv()
                    span = range(r * comp, (r + 1) * comp)
                    shift_fields(turn, plane, mixed, span.start, span.stop)
                    sums = stencil(plane, [prods[turn, at] for at in span], (r,))
                    for at, value in zip(span, sums):
                        prods[turn, at] = value
                        if turn < ITERS - 1 and plane == planes - 1:
                            basis[turn, at] = value - SHIFT * field(turn, at)
            if turn < ITERS - 1:
                pack(turn + 1)

        dots(ITERS)
        sums = jnp.sum(gram[...], axis=1)
        row = lax.dot_general(
            jnp.ones((rows, lanes), jnp.float32),
            sums,
            (((1,), (1,)), ((), ())),
            precision=lax.Precision.HIGHEST,
            preferred_element_type=jnp.float32,
        )
        part[...] = row[0:1]

        def reduce_copy(step, towards, source):
            return pltpu.make_async_remote_copy(
                src_ref=part,
                dst_ref=parts.at[source],
                send_sem=red_send.at[step],
                recv_sem=red_recv.at[step],
                device_id=towards,
                device_id_type=MESH,
            )

        if devices <= 64:
            offsets = sorted(
                itertools.product(range(count_x), range(count_y), range(count_z)),
                key=lambda at: (-min(at[1], count_y - at[1]), -at[0], at[2]),
            )
            peers = []
            for step, (ox, oy, oz) in enumerate(offsets):
                if (ox, oy, oz) == (0, 0, 0):
                    continue
                towards = (
                    lax.rem(my_x + ox, count_x), lax.rem(my_y + oy, count_y), lax.rem(my_z + oz, count_z)
                )
                from_x = lax.rem(my_x + count_x - ox, count_x)
                from_y = lax.rem(my_y + count_y - oy, count_y)
                from_z = lax.rem(my_z + count_z - oz, count_z)
                peers.append((step, towards, (from_x * count_y + from_y) * count_z + from_z))

            def for_peers(act, sending):
                for step, towards, source in peers:
                    act(reduce_copy(step, towards, me if sending else source))
        else:

            def for_peers(act, sending):
                def one(step, carry):
                    source = me if sending else lax.rem(me + devices - step, devices)
                    act(reduce_copy(step, coords(lax.rem(me + step, devices)), source))
                    return carry

                lax.fori_loop(1, devices, one, 0)

        for_peers(lambda copy: copy.start(), True)
        parts[me] = part[...]
        for_peers(lambda copy: copy.wait_recv(), False)
        found_parts = parts[...]
        count = devices
        while count > 1:
            half = count // 2
            rest = found_parts[2 * half :]
            found_parts = found_parts[:half] + found_parts[half : 2 * half]
            if count % 2:
                found_parts = jnp.concatenate([found_parts, rest], axis=0)
            count = count - half
        total_row = jnp.broadcast_to(found_parts[0], (rows, pair_pad))

        def entry(mine, other):
            slot = pair_slot[max(mine, other), min(mine, other)]
            return jnp.broadcast_to(total_row[:, slot : slot + 1], (rows, lanes))

        size = rhs * ITERS
        matrix = {}
        target = {}
        for i in range(size):
            for j in range(i + 1):
                matrix[i, j] = entry(rhs + i, rhs + j)
            for r in range(rhs):
                target[i, r] = entry(rhs + i, r)
        inverse = {}
        for k in range(size):
            inverse[k] = 1.0 / matrix[k, k]
            for i in range(k + 1, size):
                ratio = matrix[i, k] * inverse[k]
                for j in range(k + 1, i + 1):
                    matrix[i, j] = matrix[i, j] - ratio * matrix[j, k]
                for r in range(rhs):
                    target[i, r] = target[i, r] - ratio * target[k, r]
        weights = {}
        for k in range(size - 1, -1, -1):
            for r in range(rhs):
                accum = target[k, r]
                for later in range(k + 1, size):
                    accum = accum - matrix[later, k] * weights[later, r]
                weights[k, r] = accum * inverse[k]
        for r in range(rhs):
            for c in range(comp):
                found = jnp.zeros((rows, lanes), jnp.float32)
                left = right_ref[r * comp + c]
                for j in range(size):
                    found = found + weights[j, r] * field(j // rhs, (j % rhs) * comp + c)
                    left = left - weights[j, r] * prods[j // rhs, (j % rhs) * comp + c]
                sol_ref[r * comp + c] = found
                res_ref[r * comp + c] = left

        for turn in range(ITERS):
            for_each(messages(turn), lambda copy: copy.wait_send(), True)

        for_peers(lambda copy: copy.wait_send(), True)

    full = (rows, lanes)
    scratch = [
        pltpu.VMEM((fields,) + full, jnp.float32),
        pltpu.VMEM((ITERS - 1, fields) + full, jnp.float32),
        pltpu.VMEM((ITERS, fields) + full, jnp.float32),
        pltpu.VMEM((27, comp * comp) + full, jnp.bfloat16),
        pltpu.VMEM((planes, 9, comp * comp) + full, jnp.float32),
        pltpu.VMEM((9, fields) + full, jnp.float32),
        pltpu.VMEM((ITERS,) + full, jnp.float32),
        pltpu.VMEM((ITERS, 2, fields, lanes), jnp.float32),
        pltpu.VMEM((ITERS, 2, 1, lanes), jnp.float32),
        pltpu.VMEM((ITERS, planes - 1, fields) + full, jnp.float32),
        pltpu.VMEM((ITERS, planes, 2, fields, lanes), jnp.float32),
        pltpu.VMEM((ITERS, planes, 2) + full, jnp.float32),
        pltpu.VMEM((ITERS, planes, 2, 2, 1, lanes), jnp.float32),
        pltpu.VMEM((2, 3, fields, lanes), jnp.float32),
        pltpu.VMEM((pair_pad,) + full, jnp.float32),
        pltpu.VMEM((1, pair_pad), jnp.float32),
        pltpu.VMEM((devices, 1, pair_pad), jnp.float32),
        pltpu.SemaphoreType.DMA,
        pltpu.SemaphoreType.DMA,
        pltpu.SemaphoreType.DMA((ITERS, planes * slots)),
        pltpu.SemaphoreType.DMA((ITERS, planes * slots)),
        pltpu.SemaphoreType.DMA((devices,)),
        pltpu.SemaphoreType.DMA((devices,)),
    ]
    return kernel, scratch


def hand_over(found_ref, left_ref, sol_ref, res_ref, sem):
    copies = [
        pltpu.make_async_copy(found_ref, sol_ref, sem.at[0]),
        pltpu.make_async_copy(left_ref, res_ref, sem.at[1]),
    ]
    for copy in copies:
        copy.start()
    for copy in copies:
        copy.wait()


def shards(sizes, right_side, jacobian):
    rhs, comp, extent_x, rows, lanes = right_side.shape
    assert extent_x == 1
    kernel, scratch = make_kernel(sizes, rhs, comp, rows, lanes)
    shape = (rhs * comp, rows, lanes)
    vmem = pl.BlockSpec(memory_space=pltpu.VMEM)
    hbm = pl.BlockSpec(memory_space=pltpu.HBM)
    found, left = pl.pallas_call(
        kernel,
        out_shape=(pltpu.VMEM(shape, jnp.float32),) * 2,
        in_specs=[hbm, hbm],
        out_specs=(vmem, vmem),
        scratch_shapes=scratch,
        compiler_params=pltpu.CompilerParams(collective_id=0, has_side_effects=True),
    )(
        right_side.reshape(shape),
        jacobian.reshape(27, comp * comp, rows, lanes),
    )
    found, left = pl.pallas_call(
        hand_over,
        out_shape=(jax.ShapeDtypeStruct(shape, jnp.float32),) * 2,
        in_specs=[vmem, vmem],
        out_specs=(hbm, hbm),
        scratch_shapes=[pltpu.SemaphoreType.DMA((2,))],
        compiler_params=pltpu.CompilerParams(vmem_limit_bytes=24 * 2**20),
    )(found, left)
    return found.reshape(right_side.shape), left.reshape(right_side.shape)


def solution(mesh):
    sizes = tuple(mesh.shape[axis] for axis in AXES)
    in_specs = (P(None, None, *AXES), P(None, None, None, *AXES))
    out_specs = (P(None, None, *AXES), P(None, None, *AXES))
    return jax.shard_map(
        functools.partial(shards, sizes), mesh=mesh, in_specs=in_specs, out_specs=out_specs, check_vma=False
    )
```

```python
import functools
import itertools

import jax
import jax.numpy as jnp
from jax import lax
from jax.experimental import pallas as pl
from jax.experimental.pallas import tpu as pltpu
from jax.sharding import PartitionSpec as P

ITERS = 3
SHIFT = 9.0
MESH = pl.DeviceIdType.MESH
AXES = ("gx", "gy", "gz")
GROUPS = 4
KINDS = 6


def make_kernel(sizes, rhs, comp, rows, lanes):
    count_x, count_y, count_z = sizes
    devices = count_x * count_y * count_z
    fields = rhs * comp
    merged = count_x == 2
    near_only = max(count_x // 2, count_y // 2, count_z - 1) <= ITERS
    plane_steps = (0, 1) if merged else (0, 1, -1)
    planes = len(plane_steps)
    groups = GROUPS if rhs % GROUPS == 0 else rhs
    each = rhs // groups
    span = each * comp
    pair_list = []
    for mine in range(rhs, rhs * (ITERS + 1)):
        for other in range(0, mine + 1):
            pair_list.append((mine, other))
    pair_slot = {pair: slot for slot, pair in enumerate(pair_list)}
    pair_pad = -(-len(pair_list) // 128) * 128
    full = (rows, lanes)

    def kernel(
        right_hbm, jac_hbm, sol_ref, res_ref,
        right_ref, basis, prods, jac_low, jac, packs,
        far_plane, halo_rows, halo_cols, halo_corner, sums, part, parts,
        right_sem, jac_sem, send_sem, recv_sem, red_send, red_recv,
    ):
        my_x, my_y, my_z = (lax.axis_index(axis) for axis in AXES)
        me = (my_x * count_y + my_y) * count_z + my_z

        def coords(index):
            return (index // (count_y * count_z), index // count_z % count_y, index % count_z)

        def beside(step_x, dy, dz):
            return (
                lax.rem(my_x + step_x + count_x, count_x),
                lax.rem(my_y + dy + count_y, count_y),
                jnp.clip(my_z + dz, 0, count_z - 1),
            )

        above = my_z < count_z - 1
        below = my_z > 0

        def in_layer(dz, act):
            if dz == 0:
                act()
            else:
                pl.when(above if dz == 1 else below)(act)

        barrier = pltpu.get_barrier_semaphore()

        def salute(device):
            pl.semaphore_signal(barrier, inc=1, device_id=device, device_id_type=MESH)

        if near_only:
            for dz in (1, -1, 0):
                def greet_layer():
                    for step_x, dy in itertools.product(reversed(plane_steps), (1, -1, 0)):
                        if (step_x, dy, dz) != (0, 0, 0):
                            salute(beside(step_x, dy, dz))

                in_layer(dz, greet_layer)
            greeted = planes * 3 * (1 + above.astype(jnp.int32) + below.astype(jnp.int32)) - 1
        else:

            def greet(step, carry):
                salute(coords(lax.rem(me + step, devices)))
                return carry

            lax.fori_loop(1, devices, greet, 0)
            greeted = devices - 1

        right_load = pltpu.make_async_copy(right_hbm, right_ref, right_sem)
        right_load.start()
        loads = pltpu.make_async_copy(jac_hbm, jac_low, jac_sem)
        loads.start()

        lane = lax.broadcasted_iota(jnp.int32, full, 1)
        sub = lax.broadcasted_iota(jnp.int32, full, 0)

        def values(turn):
            return right_ref if turn == 0 else basis.at[turn - 1]

        def pack(turn, group, found):
            packed = jnp.zeros(full, jnp.float32)
            for at in range(span):
                packed = jnp.where(lane // 2 == at, pltpu.roll(found[at], 2 * at + 1, 1), packed)
            packs[turn, group] = packed

        def remote(source, target, kind, turn, group, device):
            return pltpu.make_async_remote_copy(
                src_ref=source,
                dst_ref=target,
                send_sem=send_sem.at[kind % KINDS],
                recv_sem=recv_sem.at[turn, group, kind],
                device_id=device,
                device_id_type=MESH,
            )

        def send(turn, group):
            mine = pl.ds(group * span, span)
            for dz in (1, -1, 0):
                side_z = 0 if dz == 1 else 1

                def layer():
                    for plane in reversed(range(planes)):
                        kind = KINDS * plane
                        for dy in (1, -1, 0):
                            device = beside(plane_steps[plane], dy, dz)
                            edge = pl.ds(rows - 1 if dy == 1 else 0, 1)
                            place = pl.ds(0 if dy == 1 else rows - 1, 1)
                            if dy == 0 and dz == 0:
                                continue
                            if dz == 0:
                                copy = remote(
                                    values(turn).at[mine, edge], halo_rows.at[turn, group, plane, :, place],
                                    kind, turn, group, device,
                                )
                            elif dy == 0:
                                copy = remote(
                                    packs.at[turn, group], halo_cols.at[turn, group, plane, side_z],
                                    kind + 1 + side_z, turn, group, device,
                                )
                            else:
                                copy = remote(
                                    packs.at[turn, group, edge], halo_corner.at[turn, group, plane, side_z, place],
                                    kind + 3 + side_z, turn, group, device,
                                )
                            copy.start()

                in_layer(dz, layer)
            for plane in range(1, planes):
                remote(
                    values(turn).at[mine], far_plane.at[turn, group, plane - 1],
                    KINDS * plane + 5, turn, group, beside(plane_steps[plane], 0, 0),
                ).start()

        def wait_edges(turn, group, plane):
            kind = KINDS * plane
            here = beside(1, 0, 0)
            both = halo_rows.at[turn, group, plane, :, pl.ds(0, 2)]
            remote(both, both, kind, turn, group, here).wait_recv()
            for side_z, dz in ((0, -1), (1, 1)):

                def layer():
                    column = halo_cols.at[turn, group, plane, side_z]
                    remote(column, column, kind + 1 + side_z, turn, group, here).wait_recv()
                    corner = halo_corner.at[turn, group, plane, side_z, pl.ds(0, 2)]
                    remote(corner, corner, kind + 3 + side_z, turn, group, here).wait_recv()

                in_layer(dz, layer)

        def wait_far(turn, group, plane):
            whole = far_plane.at[turn, group, plane - 1]
            remote(whole, whole, KINDS * plane + 5, turn, group, beside(1, 0, 0)).wait_recv()

        def turned(value, way):
            if way == 0:
                return value
            return pltpu.roll(value, 1 if way < 0 else rows - 1, 0)

        def stencil(turn, group, plane, totals):
            low = jnp.where(below, pltpu.roll(halo_cols[turn, group, plane, 0], 1, 1), 0.0)
            high = jnp.where(above, pltpu.roll(halo_cols[turn, group, plane, 1], lanes - 1, 1), 0.0)
            mixed = jnp.where(lane % 2 == 1, low, high)
            low = jnp.where(below, pltpu.roll(halo_corner[turn, group, plane, 0], 1, 1), 0.0)
            high = jnp.where(above, pltpu.roll(halo_corner[turn, group, plane, 1], lanes - 1, 1), 0.0)
            outer = jnp.where(lane % 2 == 1, low, high)
            side = {-1: sub == 0, 1: sub == rows - 1}
            columns = {0: mixed}
            for dy in (-1, 1):
                columns[dy] = jnp.where(side[dy], outer, turned(mixed, dy))
            for at in range(span):
                source = at % comp
                r = at // comp
                if plane == 0:
                    value = values(turn)[group * span + at]
                else:
                    value = far_plane[turn, group, plane - 1, at]
                beyond = halo_rows[turn, group, plane, at]
                for dy in (0, -1, 1):
                    line = value if dy == 0 else jnp.where(side[dy], beyond, turned(value, dy))
                    edge = pltpu.roll(columns[dy], lanes - 2 * at - 1, 1)
                    along = (
                        jnp.where(lane == 0, edge, pltpu.roll(line, 1, 1)),
                        line,
                        jnp.where(lane == lanes - 1, edge, pltpu.roll(line, lanes - 1, 1)),
                    )
                    for dz in range(3):
                        near = (dy + 1) * 3 + dz
                        for a in range(comp):
                            found = jac[plane, near, a * comp + source] * along[dz]
                            key = (r * comp + a, (source + dz) % 2)
                            totals[key] = totals[key] + found if key in totals else found
            return totals

        def vector(index, c):
            if index < rhs:
                return right_ref[index * comp + c]
            return prods[index // rhs - 1, (index % rhs) * comp + c]

        def dots(mine):
            own = [vector(mine, c) for c in range(comp)]
            for other in range(0, mine + 1):
                total = own[0] * vector(other, 0)
                for c in range(1, comp):
                    total = total + own[c] * vector(other, c)
                slot = pair_slot[mine, other]
                sums[slot : slot + 1, :] = jnp.sum(total, axis=0, keepdims=True)

        for slot in range(len(pair_list), pair_pad):
            sums[slot : slot + 1, :] = jnp.zeros((1, lanes), jnp.float32)
        right_load.wait()
        for group in range(groups):
            pack(0, group, [right_ref[group * span + at] for at in range(span)])
        pl.semaphore_wait(barrier, greeted)
        for group in range(groups):
            send(0, group)
        loads.wait()

        def widen(near, carry):
            for entry in range(comp * comp):
                jac[0, near, entry] = jac_low[9 + near, entry].astype(jnp.float32)
                first = jac_low[near, entry].astype(jnp.float32)
                last = jac_low[18 + near, entry].astype(jnp.float32)
                if merged:
                    jac[1, near, entry] = first + last
                else:
                    jac[1, near, entry] = first
                    jac[2, near, entry] = last
            return carry

        lax.fori_loop(0, 9, widen, 0)

        for turn in range(ITERS):
            for group in range(groups):
                totals = {}
                for plane in range(planes):
                    wait_edges(turn, group, plane)
                    if plane > 0:
                        wait_far(turn, group, plane)
                    totals = stencil(turn, group, plane, totals)
                found = [totals[at, 0] + totals[at, 1] for at in range(span)]
                for at in range(span):
                    prods[turn, group * span + at] = found[at]
                if turn < ITERS - 1:
                    found = [found[at] - SHIFT * values(turn)[group * span + at] for at in range(span)]
                    for at in range(span):
                        basis[turn, group * span + at] = found[at]
                    pack(turn + 1, group, found)
                    send(turn + 1, group)
                for r in range(group * each, (group + 1) * each):
                    dots(rhs * (turn + 1) + r)

        part[...] = jnp.sum(jnp.transpose(sums[...]), axis=0, keepdims=True)
        def reduce_copy(step, towards, source):
            return pltpu.make_async_remote_copy(
                src_ref=part,
                dst_ref=parts.at[source],
                send_sem=red_send.at[step],
                recv_sem=red_recv.at[step],
                device_id=towards,
                device_id_type=MESH,
            )

        if devices <= 64:
            offsets = sorted(
                itertools.product(range(count_x), range(count_y), range(count_z)),
                key=lambda at: (-min(at[1], count_y - at[1]), -at[0], at[2]),
            )
            peers = []
            for step, (ox, oy, oz) in enumerate(offsets):
                if (ox, oy, oz) == (0, 0, 0):
                    continue
                towards = (
                    lax.rem(my_x + ox, count_x), lax.rem(my_y + oy, count_y), lax.rem(my_z + oz, count_z)
                )
                from_x = lax.rem(my_x + count_x - ox, count_x)
                from_y = lax.rem(my_y + count_y - oy, count_y)
                from_z = lax.rem(my_z + count_z - oz, count_z)
                peers.append((step, towards, (from_x * count_y + from_y) * count_z + from_z))

            def for_peers(act, sending):
                for step, towards, source in peers:
                    act(reduce_copy(step, towards, me if sending else source))
        else:

            def for_peers(act, sending):
                def one(step, carry):
                    source = me if sending else lax.rem(me + devices - step, devices)
                    act(reduce_copy(step, coords(lax.rem(me + step, devices)), source))
                    return carry

                lax.fori_loop(1, devices, one, 0)

        for_peers(lambda copy: copy.start(), True)
        parts[me] = part[...]
        for_peers(lambda copy: copy.wait_recv(), False)
        found_parts = parts[...]
        count = devices
        while count > 1:
            half = count // 2
            rest = found_parts[2 * half :]
            found_parts = found_parts[:half] + found_parts[half : 2 * half]
            if count % 2:
                found_parts = jnp.concatenate([found_parts, rest], axis=0)
            count = count - half
        total_row = jnp.broadcast_to(found_parts[0], (rows, pair_pad))

        def entry(mine, other):
            slot = pair_slot[max(mine, other), min(mine, other)]
            return jnp.broadcast_to(total_row[:, slot : slot + 1], (rows, lanes))

        size = rhs * ITERS
        matrix = {}
        target = {}
        for i in range(size):
            for j in range(i + 1):
                matrix[i, j] = entry(rhs + i, rhs + j)
            for r in range(rhs):
                target[i, r] = entry(rhs + i, r)
        inverse = {}
        for k in range(size):
            inverse[k] = 1.0 / matrix[k, k]
            for i in range(k + 1, size):
                ratio = matrix[i, k] * inverse[k]
                for j in range(k + 1, i + 1):
                    matrix[i, j] = matrix[i, j] - ratio * matrix[j, k]
                for r in range(rhs):
                    target[i, r] = target[i, r] - ratio * target[k, r]
        weights = {}
        for k in range(size - 1, -1, -1):
            for r in range(rhs):
                accum = target[k, r]
                for later in range(k + 1, size):
                    accum = accum - matrix[later, k] * weights[later, r]
                weights[k, r] = accum * inverse[k]
        for r in range(rhs):
            for c in range(comp):
                found = jnp.zeros((rows, lanes), jnp.float32)
                left = right_ref[r * comp + c]
                for j in range(size):
                    found = found + weights[j, r] * values(j // rhs)[(j % rhs) * comp + c]
                    left = left - weights[j, r] * prods[j // rhs, (j % rhs) * comp + c]
                sol_ref[r * comp + c] = found
                res_ref[r * comp + c] = left

        for kind in range(KINDS):
            for plane in range(planes):

                def layer():
                    for turn in range(ITERS):
                        for group in range(groups):
                            if kind == 0:
                                whole = halo_rows.at[turn, group, plane, :, pl.ds(0, 2)]
                            elif kind < 3:
                                whole = halo_cols.at[turn, group, plane, kind - 1]
                            elif kind < 5:
                                whole = halo_corner.at[turn, group, plane, kind - 3, pl.ds(0, 2)]
                            elif plane > 0:
                                whole = far_plane.at[turn, group, plane - 1]
                            else:
                                continue
                            remote(whole, whole, kind, turn, group, beside(1, 0, 0)).wait_send()

                in_layer((0, 1, -1, 1, -1, 0)[kind], layer)
        for_peers(lambda copy: copy.wait_send(), True)

    copies = (ITERS, groups, planes)
    scratch = [
        pltpu.VMEM((fields,) + full, jnp.float32),
        pltpu.VMEM((ITERS - 1, fields) + full, jnp.float32),
        pltpu.VMEM((ITERS, fields) + full, jnp.float32),
        pltpu.VMEM((27, comp * comp) + full, jnp.bfloat16),
        pltpu.VMEM((planes, 9, comp * comp) + full, jnp.float32),
        pltpu.VMEM((ITERS, groups) + full, jnp.float32),
        pltpu.VMEM((ITERS, groups, planes - 1, span) + full, jnp.float32),
        pltpu.VMEM(copies + (span,) + full, jnp.float32),
        pltpu.VMEM(copies + (2,) + full, jnp.float32),
        pltpu.VMEM(copies + (2,) + full, jnp.float32),
        pltpu.VMEM((pair_pad, lanes), jnp.float32),
        pltpu.VMEM((1, pair_pad), jnp.float32),
        pltpu.VMEM((devices, 1, pair_pad), jnp.float32),
        pltpu.SemaphoreType.DMA,
        pltpu.SemaphoreType.DMA,
        pltpu.SemaphoreType.DMA((KINDS,)),
        pltpu.SemaphoreType.DMA((ITERS, groups, KINDS * planes)),
        pltpu.SemaphoreType.DMA((devices,)),
        pltpu.SemaphoreType.DMA((devices,)),
    ]
    return kernel, scratch


def hand_over(found_ref, left_ref, sol_ref, res_ref, sem):
    copies = [
        pltpu.make_async_copy(found_ref, sol_ref, sem.at[0]),
        pltpu.make_async_copy(left_ref, res_ref, sem.at[1]),
    ]
    for copy in copies:
        copy.start()
    for copy in copies:
        copy.wait()


def shards(sizes, right_side, jacobian):
    rhs, comp, extent_x, rows, lanes = right_side.shape
    assert extent_x == 1
    kernel, scratch = make_kernel(sizes, rhs, comp, rows, lanes)
    shape = (rhs * comp, rows, lanes)
    vmem = pl.BlockSpec(memory_space=pltpu.VMEM)
    hbm = pl.BlockSpec(memory_space=pltpu.HBM)
    found, left = pl.pallas_call(
        kernel,
        out_shape=(pltpu.VMEM(shape, jnp.float32),) * 2,
        in_specs=[hbm, hbm],
        out_specs=(vmem, vmem),
        scratch_shapes=scratch,
        compiler_params=pltpu.CompilerParams(collective_id=0, has_side_effects=True),
    )(
        right_side.reshape(shape),
        jacobian.reshape(27, comp * comp, rows, lanes),
    )
    found, left = pl.pallas_call(
        hand_over,
        out_shape=(jax.ShapeDtypeStruct(shape, jnp.float32),) * 2,
        in_specs=[vmem, vmem],
        out_specs=(hbm, hbm),
        scratch_shapes=[pltpu.SemaphoreType.DMA((2,))],
        compiler_params=pltpu.CompilerParams(vmem_limit_bytes=24 * 2**20),
    )(found, left)
    return found.reshape(right_side.shape), left.reshape(right_side.shape)


def solution(mesh):
    sizes = tuple(mesh.shape[axis] for axis in AXES)
    in_specs = (P(None, None, *AXES), P(None, None, None, *AXES))
    out_specs = (P(None, None, *AXES), P(None, None, *AXES))
    return jax.shard_map(
        functools.partial(shards, sizes), mesh=mesh, in_specs=in_specs, out_specs=out_specs, check_vma=False
    )
```

```python
import functools
import itertools

import jax
import jax.numpy as jnp
from jax import lax
from jax.experimental import pallas as pl
from jax.experimental.pallas import tpu as pltpu
from jax.sharding import PartitionSpec as P

ITERS = 3
SHIFT = 9.0
MESH = pl.DeviceIdType.MESH
AXES = ("gx", "gy", "gz")
GROUPS = 2
KINDS = 6


def make_kernel(sizes, rhs, comp, rows, lanes):
    count_x, count_y, count_z = sizes
    devices = count_x * count_y * count_z
    fields = rhs * comp
    merged = count_x == 2
    near_only = max(count_x // 2, count_y // 2, count_z - 1) <= ITERS
    plane_steps = (0, 1) if merged else (0, 1, -1)
    planes = len(plane_steps)
    groups = GROUPS if rhs % GROUPS == 0 else rhs
    each = rhs // groups
    span = each * comp
    pair_list = []
    for mine in range(rhs, rhs * (ITERS + 1)):
        for other in range(0, mine + 1):
            pair_list.append((mine, other))
    pair_slot = {pair: slot for slot, pair in enumerate(pair_list)}
    pair_pad = -(-len(pair_list) // 128) * 128
    full = (rows, lanes)

    def kernel(
        right_hbm, jac_hbm, sol_ref, res_ref,
        right_ref, basis, prods, jac_low, jac, packs,
        far_plane, halo_rows, halo_cols, halo_corner, sums, part, parts,
        right_sem, jac_sem, send_sem, recv_sem, red_send, red_recv,
    ):
        my_x, my_y, my_z = (lax.axis_index(axis) for axis in AXES)
        me = (my_x * count_y + my_y) * count_z + my_z

        def coords(index):
            return (index // (count_y * count_z), index // count_z % count_y, index % count_z)

        def beside(step_x, dy, dz):
            return (
                lax.rem(my_x + step_x + count_x, count_x),
                lax.rem(my_y + dy + count_y, count_y),
                jnp.clip(my_z + dz, 0, count_z - 1),
            )

        above = my_z < count_z - 1
        below = my_z > 0

        def in_layer(dz, act):
            if dz == 0:
                act()
            else:
                pl.when(above if dz == 1 else below)(act)

        barrier = pltpu.get_barrier_semaphore()

        def salute(device):
            pl.semaphore_signal(barrier, inc=1, device_id=device, device_id_type=MESH)

        if near_only:
            for dz in (1, -1, 0):
                def greet_layer():
                    for step_x, dy in itertools.product(reversed(plane_steps), (1, -1, 0)):
                        if (step_x, dy, dz) != (0, 0, 0):
                            salute(beside(step_x, dy, dz))

                in_layer(dz, greet_layer)
            greeted = planes * 3 * (1 + above.astype(jnp.int32) + below.astype(jnp.int32)) - 1
        else:

            def greet(step, carry):
                salute(coords(lax.rem(me + step, devices)))
                return carry

            lax.fori_loop(1, devices, greet, 0)
            greeted = devices - 1

        right_load = pltpu.make_async_copy(right_hbm, right_ref, right_sem)
        right_load.start()
        loads = pltpu.make_async_copy(jac_hbm, jac_low, jac_sem)
        loads.start()

        lane = lax.broadcasted_iota(jnp.int32, full, 1)
        sub = lax.broadcasted_iota(jnp.int32, full, 0)

        def values(turn):
            return right_ref if turn == 0 else basis.at[turn - 1]

        def pack(turn, group, found):
            packed = jnp.zeros(full, jnp.float32)
            for at in range(span):
                packed = jnp.where(lane // 2 == at, pltpu.roll(found[at], 2 * at + 1, 1), packed)
            packs[turn, group] = packed

        def remote(source, target, kind, turn, group, device):
            return pltpu.make_async_remote_copy(
                src_ref=source,
                dst_ref=target,
                send_sem=send_sem.at[kind % KINDS],
                recv_sem=recv_sem.at[turn % 2, group, kind],
                device_id=device,
                device_id_type=MESH,
            )

        def send(turn, group):
            mine = pl.ds(group * span, span)
            for dz in (1, -1, 0):
                side_z = 0 if dz == 1 else 1

                def layer():
                    for plane in reversed(range(planes)):
                        kind = KINDS * plane
                        for dy in (1, -1, 0):
                            device = beside(plane_steps[plane], dy, dz)
                            edge = pl.ds(rows - 1 if dy == 1 else 0, 1)
                            place = pl.ds(0 if dy == 1 else rows - 1, 1)
                            if dy == 0 and dz == 0:
                                continue
                            if dz == 0:
                                copy = remote(
                                    values(turn).at[mine, edge], halo_rows.at[turn, group, plane, :, place],
                                    kind, turn, group, device,
                                )
                            elif dy == 0:
                                copy = remote(
                                    packs.at[turn, group], halo_cols.at[turn, group, plane, side_z],
                                    kind + 1 + side_z, turn, group, device,
                                )
                            else:
                                copy = remote(
                                    packs.at[turn, group, edge], halo_corner.at[turn, group, plane, side_z, place],
                                    kind + 3 + side_z, turn, group, device,
                                )
                            copy.start()

                in_layer(dz, layer)
            for plane in range(1, planes):
                remote(
                    values(turn).at[mine], far_plane.at[turn, group, plane - 1],
                    KINDS * plane + 5, turn, group, beside(plane_steps[plane], 0, 0),
                ).start()

        def wait_edges(turn, group, plane):
            kind = KINDS * plane
            here = beside(1, 0, 0)
            both = halo_rows.at[turn, group, plane, :, pl.ds(0, 2)]
            remote(both, both, kind, turn, group, here).wait_recv()
            for side_z, dz in ((0, -1), (1, 1)):

                def layer():
                    column = halo_cols.at[turn, group, plane, side_z]
                    remote(column, column, kind + 1 + side_z, turn, group, here).wait_recv()
                    corner = halo_corner.at[turn, group, plane, side_z, pl.ds(0, 2)]
                    remote(corner, corner, kind + 3 + side_z, turn, group, here).wait_recv()

                in_layer(dz, layer)

        def wait_far(turn, group, plane):
            whole = far_plane.at[turn, group, plane - 1]
            remote(whole, whole, KINDS * plane + 5, turn, group, beside(1, 0, 0)).wait_recv()

        def turned(value, way):
            if way == 0:
                return value
            return pltpu.roll(value, 1 if way < 0 else rows - 1, 0)

        def stencil(turn, group, plane, totals):
            low = jnp.where(below, pltpu.roll(halo_cols[turn, group, plane, 0], 1, 1), 0.0)
            high = jnp.where(above, pltpu.roll(halo_cols[turn, group, plane, 1], lanes - 1, 1), 0.0)
            mixed = jnp.where(lane % 2 == 1, low, high)
            low = jnp.where(below, pltpu.roll(halo_corner[turn, group, plane, 0], 1, 1), 0.0)
            high = jnp.where(above, pltpu.roll(halo_corner[turn, group, plane, 1], lanes - 1, 1), 0.0)
            outer = jnp.where(lane % 2 == 1, low, high)
            side = {-1: sub == 0, 1: sub == rows - 1}
            columns = {0: mixed}
            for dy in (-1, 1):
                columns[dy] = jnp.where(side[dy], outer, turned(mixed, dy))
            for at in range(span):
                source = at % comp
                r = at // comp
                if plane == 0:
                    value = values(turn)[group * span + at]
                else:
                    value = far_plane[turn, group, plane - 1, at]
                beyond = halo_rows[turn, group, plane, at]
                for dy in (0, -1, 1):
                    line = value if dy == 0 else jnp.where(side[dy], beyond, turned(value, dy))
                    edge = pltpu.roll(columns[dy], lanes - 2 * at - 1, 1)
                    along = (
                        jnp.where(lane == 0, edge, pltpu.roll(line, 1, 1)),
                        line,
                        jnp.where(lane == lanes - 1, edge, pltpu.roll(line, lanes - 1, 1)),
                    )
                    for dz in range(3):
                        near = (dy + 1) * 3 + dz
                        for a in range(comp):
                            found = jac[plane, near, a * comp + source] * along[dz]
                            key = (r * comp + a, (source + dz) % 2)
                            totals[key] = totals[key] + found if key in totals else found
            return totals

        def vector(index, c):
            if index < rhs:
                return right_ref[index * comp + c]
            return prods[index // rhs - 1, (index % rhs) * comp + c]

        def dots(mine):
            own = [vector(mine, c) for c in range(comp)]
            for other in range(0, mine + 1):
                total = own[0] * vector(other, 0)
                for c in range(1, comp):
                    total = total + own[c] * vector(other, c)
                slot = pair_slot[mine, other]
                sums[slot : slot + 1, :] = jnp.sum(total, axis=0, keepdims=True)

        for slot in range(len(pair_list), pair_pad):
            sums[slot : slot + 1, :] = jnp.zeros((1, lanes), jnp.float32)
        right_load.wait()
        for group in range(groups):
            pack(0, group, [right_ref[group * span + at] for at in range(span)])
        pl.semaphore_wait(barrier, greeted)
        for group in range(groups):
            send(0, group)
        loads.wait()

        def widen(near, carry):
            for entry in range(comp * comp):
                jac[0, near, entry] = jac_low[9 + near, entry].astype(jnp.float32)
                first = jac_low[near, entry].astype(jnp.float32)
                last = jac_low[18 + near, entry].astype(jnp.float32)
                if merged:
                    jac[1, near, entry] = first + last
                else:
                    jac[1, near, entry] = first
                    jac[2, near, entry] = last
            return carry

        lax.fori_loop(0, 9, widen, 0)

        for turn in range(ITERS):
            for group in range(groups):
                wait_edges(turn, group, 0)
                totals = stencil(turn, group, 0, {})
                for at in range(span):
                    prods[turn, group * span + at] = totals[at, 0] + totals[at, 1]
            for group in range(groups):
                totals = {(at, 0): prods[turn, group * span + at] for at in range(span)}
                for plane in range(1, planes):
                    wait_edges(turn, group, plane)
                    wait_far(turn, group, plane)
                    totals = stencil(turn, group, plane, totals)
                found = [totals[at, 0] + totals[at, 1] for at in range(span)]
                for at in range(span):
                    prods[turn, group * span + at] = found[at]
                if turn < ITERS - 1:
                    found = [found[at] - SHIFT * values(turn)[group * span + at] for at in range(span)]
                    for at in range(span):
                        basis[turn, group * span + at] = found[at]
                    pack(turn + 1, group, found)
                    send(turn + 1, group)
                else:
                    for r in range(group * each, (group + 1) * each):
                        dots(rhs * (turn + 1) + r)
            if turn < ITERS - 1:
                for r in range(rhs):
                    dots(rhs * (turn + 1) + r)

        part[...] = jnp.sum(jnp.transpose(sums[...]), axis=0, keepdims=True)
        def reduce_copy(towards, source, target):
            return pltpu.make_async_remote_copy(
                src_ref=source,
                dst_ref=target,
                send_sem=red_send,
                recv_sem=red_recv,
                device_id=towards,
                device_id_type=MESH,
            )

        if devices <= 64:
            offsets = sorted(
                itertools.product(range(count_x), range(count_y), range(count_z)),
                key=lambda at: (-min(at[1], count_y - at[1]), -at[0], at[2]),
            )
            for ox, oy, oz in offsets:
                if (ox, oy, oz) != (0, 0, 0):
                    towards = (
                        lax.rem(my_x + ox, count_x), lax.rem(my_y + oy, count_y), lax.rem(my_z + oz, count_z)
                    )
                    reduce_copy(towards, part, parts.at[me]).start()
        else:

            def begin(step, carry):
                reduce_copy(coords(lax.rem(me + step, devices)), part, parts.at[me]).start()
                return carry

            lax.fori_loop(1, devices, begin, 0)
        parts[me] = part[...]
        for kind in range(KINDS):
            for plane in range(planes):

                def layer():
                    for turn in range(ITERS):
                        for group in range(groups):
                            if kind == 0:
                                whole = halo_rows.at[turn, group, plane, :, pl.ds(0, 2)]
                            elif kind < 3:
                                whole = halo_cols.at[turn, group, plane, kind - 1]
                            elif kind < 5:
                                whole = halo_corner.at[turn, group, plane, kind - 3, pl.ds(0, 2)]
                            elif plane > 0:
                                whole = far_plane.at[turn, group, plane - 1]
                            else:
                                continue
                            remote(whole, whole, kind, turn, group, beside(1, 0, 0)).wait_send()

                in_layer((0, 1, -1, 1, -1, 0)[kind], layer)
        others = parts.at[pl.ds(0, devices - 1)]
        all_others = reduce_copy(beside(1, 0, 0), others, others)
        all_others.wait_recv()
        all_others.wait_send()
        found_parts = parts[...]
        count = devices
        while count > 1:
            half = count // 2
            rest = found_parts[2 * half :]
            found_parts = found_parts[:half] + found_parts[half : 2 * half]
            if count % 2:
                found_parts = jnp.concatenate([found_parts, rest], axis=0)
            count = count - half
        total_row = jnp.broadcast_to(found_parts[0], (rows, pair_pad))

        def entry(mine, other):
            slot = pair_slot[max(mine, other), min(mine, other)]
            return jnp.broadcast_to(total_row[:, slot : slot + 1], (rows, lanes))

        size = rhs * ITERS
        matrix = {}
        target = {}
        for i in range(size):
            for j in range(i + 1):
                matrix[i, j] = entry(rhs + i, rhs + j)
            for r in range(rhs):
                target[i, r] = entry(rhs + i, r)
        inverse = {}
        for k in range(size):
            inverse[k] = 1.0 / matrix[k, k]
            for i in range(k + 1, size):
                ratio = matrix[i, k] * inverse[k]
                for j in range(k + 1, i + 1):
                    matrix[i, j] = matrix[i, j] - ratio * matrix[j, k]
                for r in range(rhs):
                    target[i, r] = target[i, r] - ratio * target[k, r]
        weights = {}
        for k in range(size - 1, -1, -1):
            for r in range(rhs):
                weights[k, r] = target[k, r] * inverse[k]
                for prior in range(k):
                    target[prior, r] = target[prior, r] - matrix[k, prior] * weights[k, r]
        for r in range(rhs):
            for c in range(comp):
                found = jnp.zeros((rows, lanes), jnp.float32)
                left = right_ref[r * comp + c]
                for j in range(size - 1, -1, -1):
                    found = found + weights[j, r] * values(j // rhs)[(j % rhs) * comp + c]
                    left = left - weights[j, r] * prods[j // rhs, (j % rhs) * comp + c]
                sol_ref[r * comp + c] = found
                res_ref[r * comp + c] = left

    copies = (ITERS, groups, planes)
    scratch = [
        pltpu.VMEM((fields,) + full, jnp.float32),
        pltpu.VMEM((ITERS - 1, fields) + full, jnp.float32),
        pltpu.VMEM((ITERS, fields) + full, jnp.float32),
        pltpu.VMEM((27, comp * comp) + full, jnp.bfloat16),
        pltpu.VMEM((planes, 9, comp * comp) + full, jnp.float32),
        pltpu.VMEM((ITERS, groups) + full, jnp.float32),
        pltpu.VMEM((ITERS, groups, planes - 1, span) + full, jnp.float32),
        pltpu.VMEM(copies + (span,) + full, jnp.float32),
        pltpu.VMEM(copies + (2,) + full, jnp.float32),
        pltpu.VMEM(copies + (2,) + full, jnp.float32),
        pltpu.VMEM((pair_pad, lanes), jnp.float32),
        pltpu.VMEM((1, pair_pad), jnp.float32),
        pltpu.VMEM((devices, 1, pair_pad), jnp.float32),
        pltpu.SemaphoreType.DMA,
        pltpu.SemaphoreType.DMA,
        pltpu.SemaphoreType.DMA((KINDS,)),
        pltpu.SemaphoreType.DMA((2, groups, KINDS * planes)),
        pltpu.SemaphoreType.DMA,
        pltpu.SemaphoreType.DMA,
    ]
    return kernel, scratch


def hand_over(found_ref, left_ref, sol_ref, res_ref, sem):
    copies = [
        pltpu.make_async_copy(found_ref, sol_ref, sem.at[0]),
        pltpu.make_async_copy(left_ref, res_ref, sem.at[1]),
    ]
    for copy in copies:
        copy.start()
    for copy in copies:
        copy.wait()


def shards(sizes, right_side, jacobian):
    rhs, comp, extent_x, rows, lanes = right_side.shape
    assert extent_x == 1
    kernel, scratch = make_kernel(sizes, rhs, comp, rows, lanes)
    shape = (rhs * comp, rows, lanes)
    vmem = pl.BlockSpec(memory_space=pltpu.VMEM)
    hbm = pl.BlockSpec(memory_space=pltpu.HBM)
    found, left = pl.pallas_call(
        kernel,
        out_shape=(pltpu.VMEM(shape, jnp.float32),) * 2,
        in_specs=[hbm, hbm],
        out_specs=(vmem, vmem),
        scratch_shapes=scratch,
        compiler_params=pltpu.CompilerParams(collective_id=0, has_side_effects=True),
    )(
        right_side.reshape(shape),
        jacobian.reshape(27, comp * comp, rows, lanes),
    )
    found, left = pl.pallas_call(
        hand_over,
        out_shape=(jax.ShapeDtypeStruct(shape, jnp.float32),) * 2,
        in_specs=[vmem, vmem],
        out_specs=(hbm, hbm),
        scratch_shapes=[pltpu.SemaphoreType.DMA((2,))],
        compiler_params=pltpu.CompilerParams(vmem_limit_bytes=24 * 2**20),
    )(found, left)
    return found.reshape(right_side.shape), left.reshape(right_side.shape)


def solution(mesh):
    sizes = tuple(mesh.shape[axis] for axis in AXES)
    in_specs = (P(None, None, *AXES), P(None, None, None, *AXES))
    out_specs = (P(None, None, *AXES), P(None, None, *AXES))
    return jax.shard_map(
        functools.partial(shards, sizes), mesh=mesh, in_specs=in_specs, out_specs=out_specs, check_vma=False
    )
```

```python
import functools
import itertools

import jax
import jax.numpy as jnp
from jax import lax
from jax.experimental import pallas as pl
from jax.experimental.pallas import tpu as pltpu
from jax.sharding import PartitionSpec as P

ITERS = 3
SHIFT = 9.0
MESH = pl.DeviceIdType.MESH
AXES = ("gx", "gy", "gz")
GROUPS = 2
KINDS = 6


def make_kernel(sizes, rhs, comp, rows, lanes):
    count_x, count_y, count_z = sizes
    devices = count_x * count_y * count_z
    fields = rhs * comp
    merged = count_x == 2
    near_only = max(count_x // 2, count_y // 2, count_z - 1) <= ITERS
    plane_steps = (0, 1) if merged else (0, 1, -1)
    planes = len(plane_steps)
    groups = GROUPS if rhs % GROUPS == 0 else rhs
    each = rhs // groups
    span = each * comp
    pair_list = []
    for mine in range(rhs, rhs * (ITERS + 1)):
        for other in range(0, mine + 1):
            pair_list.append((mine, other))
    pair_slot = {pair: slot for slot, pair in enumerate(pair_list)}
    pair_pad = -(-len(pair_list) // 128) * 128
    full = (rows, lanes)

    def kernel(
        right_hbm, jac_hbm, sol_ref, res_ref,
        right_ref, basis, prods, partial, jac_low, jac, packs,
        far_plane, halo_rows, halo_cols, halo_corner, sums, part, parts,
        right_sem, jac_sem, send_sem, recv_sem, red_send, red_recv,
    ):
        my_x, my_y, my_z = (lax.axis_index(axis) for axis in AXES)
        me = (my_x * count_y + my_y) * count_z + my_z

        def coords(index):
            return (index // (count_y * count_z), index // count_z % count_y, index % count_z)

        def beside(step_x, dy, dz):
            return (
                lax.rem(my_x + step_x + count_x, count_x),
                lax.rem(my_y + dy + count_y, count_y),
                jnp.clip(my_z + dz, 0, count_z - 1),
            )

        above = my_z < count_z - 1
        below = my_z > 0

        def in_layer(dz, act):
            if dz == 0:
                act()
            else:
                pl.when(above if dz == 1 else below)(act)

        barrier = pltpu.get_barrier_semaphore()

        def salute(device):
            pl.semaphore_signal(barrier, inc=1, device_id=device, device_id_type=MESH)

        if near_only:
            for dz in (1, -1, 0):
                def greet_layer():
                    for step_x, dy in itertools.product(reversed(plane_steps), (1, -1, 0)):
                        if (step_x, dy, dz) != (0, 0, 0):
                            salute(beside(step_x, dy, dz))

                in_layer(dz, greet_layer)
            greeted = planes * 3 * (1 + above.astype(jnp.int32) + below.astype(jnp.int32)) - 1
        else:

            def greet(step, carry):
                salute(coords(lax.rem(me + step, devices)))
                return carry

            lax.fori_loop(1, devices, greet, 0)
            greeted = devices - 1

        right_load = pltpu.make_async_copy(right_hbm, right_ref, right_sem)
        right_load.start()
        loads = pltpu.make_async_copy(jac_hbm, jac_low, jac_sem)
        loads.start()

        lane = lax.broadcasted_iota(jnp.int32, full, 1)
        sub = lax.broadcasted_iota(jnp.int32, full, 0)

        def values(turn):
            return right_ref if turn == 0 else basis.at[turn - 1]

        def pack(turn, group, found):
            packed = jnp.zeros(full, jnp.float32)
            for at in range(span):
                packed = jnp.where(lane // 2 == at, pltpu.roll(found[at], 2 * at + 1, 1), packed)
            packs[turn, group] = packed

        def remote(source, target, kind, turn, group, device):
            return pltpu.make_async_remote_copy(
                src_ref=source,
                dst_ref=target,
                send_sem=send_sem.at[kind % KINDS],
                recv_sem=recv_sem.at[turn % 2, group, kind],
                device_id=device,
                device_id_type=MESH,
            )

        def send(turn, group):
            mine = pl.ds(group * span, span)
            for dz in (1, -1, 0):
                side_z = 0 if dz == 1 else 1

                def layer():
                    for plane in reversed(range(planes)):
                        kind = KINDS * plane
                        for dy in (1, -1, 0):
                            device = beside(plane_steps[plane], dy, dz)
                            edge = pl.ds(rows - 1 if dy == 1 else 0, 1)
                            place = pl.ds(0 if dy == 1 else rows - 1, 1)
                            if dy == 0 and dz == 0:
                                continue
                            if dz == 0:
                                copy = remote(
                                    values(turn).at[mine, edge], halo_rows.at[turn, group, plane, :, place],
                                    kind, turn, group, device,
                                )
                            elif dy == 0:
                                copy = remote(
                                    packs.at[turn, group], halo_cols.at[turn, group, plane, side_z],
                                    kind + 1 + side_z, turn, group, device,
                                )
                            else:
                                copy = remote(
                                    packs.at[turn, group, edge], halo_corner.at[turn, group, plane, side_z, place],
                                    kind + 3 + side_z, turn, group, device,
                                )
                            copy.start()

                in_layer(dz, layer)
            for plane in range(1, planes):
                remote(
                    values(turn).at[mine], far_plane.at[turn, group, plane - 1],
                    KINDS * plane + 5, turn, group, beside(plane_steps[plane], 0, 0),
                ).start()

        def wait_edges(turn, group, plane):
            kind = KINDS * plane
            here = beside(1, 0, 0)
            both = halo_rows.at[turn, group, plane, :, pl.ds(0, 2)]
            remote(both, both, kind, turn, group, here).wait_recv()
            for side_z, dz in ((0, -1), (1, 1)):

                def layer():
                    column = halo_cols.at[turn, group, plane, side_z]
                    remote(column, column, kind + 1 + side_z, turn, group, here).wait_recv()
                    corner = halo_corner.at[turn, group, plane, side_z, pl.ds(0, 2)]
                    remote(corner, corner, kind + 3 + side_z, turn, group, here).wait_recv()

                in_layer(dz, layer)

        def wait_far(turn, group, plane):
            whole = far_plane.at[turn, group, plane - 1]
            remote(whole, whole, KINDS * plane + 5, turn, group, beside(1, 0, 0)).wait_recv()

        def turned(value, way):
            if way == 0:
                return value
            return pltpu.roll(value, 1 if way < 0 else rows - 1, 0)

        def stencil(turn, group, plane, totals):
            even = lane % 2 == 0

            def edges(halo):
                low = jnp.where(below, halo[turn, group, plane, 0], 0.0)
                high = jnp.where(above, halo[turn, group, plane, 1], 0.0)
                return jnp.where(even, low, high)

            inner, outer = edges(halo_cols), edges(halo_corner)
            side = {-1: sub == 0, 1: sub == rows - 1}
            columns = {dy: jnp.where(side[dy], outer, turned(inner, dy)) for dy in (-1, 1)}
            columns[0] = inner
            for source in range(comp):
                for dy in (0, -1, 1):
                    along = {}
                    for r in range(each):
                        at = r * comp + source
                        if plane == 0:
                            value = values(turn)[group * span + at]
                        else:
                            value = far_plane[turn, group, plane - 1, at]
                        if dy != 0:
                            value = jnp.where(side[dy], halo_rows[turn, group, plane, at], turned(value, dy))
                        edge = pltpu.roll(columns[dy], lanes - 2 * at - 1, 1)
                        along[r, 1] = value
                        along[r, 0] = jnp.where(lane == lanes - 1, edge, value)
                        along[r, 2] = jnp.where(lane == 0, edge, value)
                    for dz in (1, 0, 2):
                        near = (dy + 1) * 3 + dz
                        for a in range(comp):
                            block = jac[plane, near, a * comp + source]
                            for r in range(each):
                                found = block * along[r, dz]
                                key = (r * comp + a, dz)
                                totals[key] = totals[key] + found if key in totals else found
            return totals

        def joined(totals):
            return [
                totals[at, 1] + (pltpu.roll(totals[at, 0], 1, 1) + pltpu.roll(totals[at, 2], lanes - 1, 1))
                for at in range(span)
            ]

        def vector(index, c):
            if index < rhs:
                return right_ref[index * comp + c]
            return prods[index // rhs - 1, (index % rhs) * comp + c]

        def dots(mine):
            own = [vector(mine, c) for c in range(comp)]
            for other in range(0, mine + 1):
                total = own[0] * vector(other, 0)
                for c in range(1, comp):
                    total = total + own[c] * vector(other, c)
                slot = pair_slot[mine, other]
                sums[slot : slot + 1, :] = jnp.sum(total, axis=0, keepdims=True)

        for slot in range(len(pair_list), pair_pad):
            sums[slot : slot + 1, :] = jnp.zeros((1, lanes), jnp.float32)
        right_load.wait()
        for group in range(groups):
            pack(0, group, [right_ref[group * span + at] for at in range(span)])
        pl.semaphore_wait(barrier, greeted)
        for group in range(groups):
            send(0, group)
        loads.wait()

        def widen(line, carry):
            for dz, shift in enumerate((lanes - 1, 0, 1)):
                near = line * 3 + dz

                def block(step_x, entry):
                    found = jac_low[9 * step_x + near, entry].astype(jnp.float32)
                    return pltpu.roll(found, shift, 1) if shift else found

                for entry in range(comp * comp):
                    jac[0, near, entry] = block(1, entry)
                    if merged:
                        found = jac_low[near, entry].astype(jnp.float32) + jac_low[18 + near, entry].astype(jnp.float32)
                        jac[1, near, entry] = pltpu.roll(found, shift, 1) if shift else found
                    else:
                        jac[1, near, entry] = block(0, entry)
                        jac[2, near, entry] = block(2, entry)
            return carry

        lax.fori_loop(0, 3, widen, 0)

        for turn in range(ITERS):
            for group in range(groups):
                wait_edges(turn, group, 0)
                totals = stencil(turn, group, 0, {})
                for (at, dz), total in totals.items():
                    partial[group, dz, at] = total
            for group in range(groups):
                totals = {(at, dz): partial[group, dz, at] for at in range(span) for dz in range(3)}
                for plane in range(1, planes):
                    wait_edges(turn, group, plane)
                    wait_far(turn, group, plane)
                    totals = stencil(turn, group, plane, totals)
                found = joined(totals)
                for at in range(span):
                    prods[turn, group * span + at] = found[at]
                if turn < ITERS - 1:
                    found = [found[at] - SHIFT * values(turn)[group * span + at] for at in range(span)]
                    for at in range(span):
                        basis[turn, group * span + at] = found[at]
                    pack(turn + 1, group, found)
                    send(turn + 1, group)
                else:
                    for r in range(group * each, (group + 1) * each):
                        dots(rhs * (turn + 1) + r)
            if turn < ITERS - 1:
                for r in range(rhs):
                    dots(rhs * (turn + 1) + r)

        part[...] = jnp.sum(jnp.transpose(sums[...]), axis=0, keepdims=True)
        def reduce_copy(towards, source, target):
            return pltpu.make_async_remote_copy(
                src_ref=source,
                dst_ref=target,
                send_sem=red_send,
                recv_sem=red_recv,
                device_id=towards,
                device_id_type=MESH,
            )

        if devices <= 64:
            offsets = sorted(
                itertools.product(range(count_x), range(count_y), range(count_z)),
                key=lambda at: (-min(at[1], count_y - at[1]), -at[0], at[2]),
            )
            for ox, oy, oz in offsets:
                if (ox, oy, oz) != (0, 0, 0):
                    towards = (
                        lax.rem(my_x + ox, count_x), lax.rem(my_y + oy, count_y), lax.rem(my_z + oz, count_z)
                    )
                    reduce_copy(towards, part, parts.at[me]).start()
        else:

            def begin(step, carry):
                reduce_copy(coords(lax.rem(me + step, devices)), part, parts.at[me]).start()
                return carry

            lax.fori_loop(1, devices, begin, 0)
        parts[me] = part[...]
        for kind in range(KINDS):
            for plane in range(planes):

                def layer():
                    for turn in range(ITERS):
                        for group in range(groups):
                            if kind == 0:
                                whole = halo_rows.at[turn, group, plane, :, pl.ds(0, 2)]
                            elif kind < 3:
                                whole = halo_cols.at[turn, group, plane, kind - 1]
                            elif kind < 5:
                                whole = halo_corner.at[turn, group, plane, kind - 3, pl.ds(0, 2)]
                            elif plane > 0:
                                whole = far_plane.at[turn, group, plane - 1]
                            else:
                                continue
                            remote(whole, whole, kind, turn, group, beside(1, 0, 0)).wait_send()

                in_layer((0, 1, -1, 1, -1, 0)[kind], layer)
        others = parts.at[pl.ds(0, devices - 1)]
        all_others = reduce_copy(beside(1, 0, 0), others, others)
        all_others.wait_recv()
        all_others.wait_send()
        found_parts = parts[...]
        count = devices
        while count > 1:
            half = count // 2
            rest = found_parts[2 * half :]
            found_parts = found_parts[:half] + found_parts[half : 2 * half]
            if count % 2:
                found_parts = jnp.concatenate([found_parts, rest], axis=0)
            count = count - half
        total_row = jnp.broadcast_to(found_parts[0], (rows, pair_pad))

        def entry(mine, other):
            slot = pair_slot[max(mine, other), min(mine, other)]
            return jnp.broadcast_to(total_row[:, slot : slot + 1], (rows, lanes))

        size = rhs * ITERS
        matrix = {}
        target = {}
        for i in range(size):
            for j in range(i + 1):
                matrix[i, j] = entry(rhs + i, rhs + j)
            for r in range(rhs):
                target[i, r] = entry(rhs + i, r)
        inverse = {}
        for k in range(size):
            inverse[k] = 1.0 / matrix[k, k]
            for i in range(k + 1, size):
                ratio = matrix[i, k] * inverse[k]
                for j in range(k + 1, i + 1):
                    matrix[i, j] = matrix[i, j] - ratio * matrix[j, k]
                for r in range(rhs):
                    target[i, r] = target[i, r] - ratio * target[k, r]
        weights = {}
        for k in range(size - 1, -1, -1):
            for r in range(rhs):
                weights[k, r] = target[k, r] * inverse[k]
                for prior in range(k):
                    target[prior, r] = target[prior, r] - matrix[k, prior] * weights[k, r]
        for c in range(comp):
            found = {}
            left = {r: right_ref[r * comp + c] for r in range(rhs)}
            for j in range(size - 1, -1, -1):
                direction = values(j // rhs)[(j % rhs) * comp + c]
                product = prods[j // rhs, (j % rhs) * comp + c]
                for r in range(rhs):
                    term = weights[j, r] * direction
                    found[r] = found[r] + term if r in found else term
                    left[r] = left[r] - weights[j, r] * product
            for r in range(rhs):
                sol_ref[r * comp + c] = found[r]
                res_ref[r * comp + c] = left[r]

    copies = (ITERS, groups, planes)
    scratch = [
        pltpu.VMEM((fields,) + full, jnp.float32),
        pltpu.VMEM((ITERS - 1, fields) + full, jnp.float32),
        pltpu.VMEM((ITERS, fields) + full, jnp.float32),
        pltpu.VMEM((groups, 3, span) + full, jnp.float32),
        pltpu.VMEM((27, comp * comp) + full, jnp.bfloat16),
        pltpu.VMEM((planes, 9, comp * comp) + full, jnp.float32),
        pltpu.VMEM((ITERS, groups) + full, jnp.float32),
        pltpu.VMEM((ITERS, groups, planes - 1, span) + full, jnp.float32),
        pltpu.VMEM(copies + (span,) + full, jnp.float32),
        pltpu.VMEM(copies + (2,) + full, jnp.float32),
        pltpu.VMEM(copies + (2,) + full, jnp.float32),
        pltpu.VMEM((pair_pad, lanes), jnp.float32),
        pltpu.VMEM((1, pair_pad), jnp.float32),
        pltpu.VMEM((devices, 1, pair_pad), jnp.float32),
        pltpu.SemaphoreType.DMA,
        pltpu.SemaphoreType.DMA,
        pltpu.SemaphoreType.DMA((KINDS,)),
        pltpu.SemaphoreType.DMA((2, groups, KINDS * planes)),
        pltpu.SemaphoreType.DMA,
        pltpu.SemaphoreType.DMA,
    ]
    return kernel, scratch


def hand_over(found_ref, left_ref, sol_ref, res_ref, sem):
    copies = [
        pltpu.make_async_copy(found_ref, sol_ref, sem.at[0]),
        pltpu.make_async_copy(left_ref, res_ref, sem.at[1]),
    ]
    for copy in copies:
        copy.start()
    for copy in copies:
        copy.wait()


def shards(sizes, right_side, jacobian):
    rhs, comp, extent_x, rows, lanes = right_side.shape
    assert extent_x == 1
    kernel, scratch = make_kernel(sizes, rhs, comp, rows, lanes)
    shape = (rhs * comp, rows, lanes)
    vmem = pl.BlockSpec(memory_space=pltpu.VMEM)
    hbm = pl.BlockSpec(memory_space=pltpu.HBM)
    found, left = pl.pallas_call(
        kernel,
        out_shape=(pltpu.VMEM(shape, jnp.float32),) * 2,
        in_specs=[hbm, hbm],
        out_specs=(vmem, vmem),
        scratch_shapes=scratch,
        compiler_params=pltpu.CompilerParams(collective_id=0, has_side_effects=True),
    )(
        right_side.reshape(shape),
        jacobian.reshape(27, comp * comp, rows, lanes),
    )
    found, left = pl.pallas_call(
        hand_over,
        out_shape=(jax.ShapeDtypeStruct(shape, jnp.float32),) * 2,
        in_specs=[vmem, vmem],
        out_specs=(hbm, hbm),
        scratch_shapes=[pltpu.SemaphoreType.DMA((2,))],
        compiler_params=pltpu.CompilerParams(vmem_limit_bytes=24 * 2**20),
    )(found, left)
    return found.reshape(right_side.shape), left.reshape(right_side.shape)


def solution(mesh):
    sizes = tuple(mesh.shape[axis] for axis in AXES)
    in_specs = (P(None, None, *AXES), P(None, None, None, *AXES))
    out_specs = (P(None, None, *AXES), P(None, None, *AXES))
    return jax.shard_map(
        functools.partial(shards, sizes), mesh=mesh, in_specs=in_specs, out_specs=out_specs, check_vma=False
    )
```

```python
import functools
import itertools

import jax
import jax.numpy as jnp
from jax import lax
from jax.experimental import pallas as pl
from jax.experimental.pallas import tpu as pltpu
from jax.sharding import PartitionSpec as P

ITERS = 3
SHIFT = 9.0
MESH = pl.DeviceIdType.MESH
AXES = ("gx", "gy", "gz")
GROUPS = 2
KINDS = 5


def make_kernel(sizes, rhs, comp, rows, lanes):
    count_x, count_y, count_z = sizes
    devices = count_x * count_y * count_z
    fields = rhs * comp
    merged = count_x == 2
    near_only = max(count_x // 2, count_y // 2, count_z - 1) <= ITERS
    plane_steps = (0, 1) if merged else (0, 1, -1)
    planes = len(plane_steps)
    groups = GROUPS if rhs % GROUPS == 0 else rhs
    each = rhs // groups
    span = each * comp
    pair_list = []
    for mine in range(rhs, rhs * (ITERS + 1)):
        for other in range(0, mine + 1):
            pair_list.append((mine, other))
    pair_slot = {pair: slot for slot, pair in enumerate(pair_list)}
    pair_pad = -(-len(pair_list) // 128) * 128
    full = (rows, lanes)

    def kernel(
        right_hbm, jac_hbm, sol_ref, res_ref,
        right_ref, basis, prods, partial, jac_low, jac, packs,
        far_plane, halo_rows, halo_cols, halo_corner, sums, part, parts,
        right_sem, jac_sem, send_sem, recv_sem, red_send, red_recv,
    ):
        my_x, my_y, my_z = (lax.axis_index(axis) for axis in AXES)
        me = (my_x * count_y + my_y) * count_z + my_z

        def coords(index):
            return (index // (count_y * count_z), index // count_z % count_y, index % count_z)

        def beside(step_x, dy, dz):
            return (
                lax.rem(my_x + step_x + count_x, count_x),
                lax.rem(my_y + dy + count_y, count_y),
                jnp.clip(my_z + dz, 0, count_z - 1),
            )

        above = my_z < count_z - 1
        below = my_z > 0

        def in_layer(dz, act):
            if dz == 0:
                act()
            else:
                pl.when(above if dz == 1 else below)(act)

        barrier = pltpu.get_barrier_semaphore()

        def salute(device):
            pl.semaphore_signal(barrier, inc=1, device_id=device, device_id_type=MESH)

        if near_only:
            for dz in (1, -1, 0):
                def greet_layer():
                    for step_x, dy in itertools.product(reversed(plane_steps), (1, -1, 0)):
                        if (step_x, dy, dz) != (0, 0, 0):
                            salute(beside(step_x, dy, dz))

                in_layer(dz, greet_layer)
            greeted = planes * 3 * (1 + above.astype(jnp.int32) + below.astype(jnp.int32)) - 1
        else:

            def greet(step, carry):
                salute(coords(lax.rem(me + step, devices)))
                return carry

            lax.fori_loop(1, devices, greet, 0)
            greeted = devices - 1

        right_load = pltpu.make_async_copy(right_hbm, right_ref, right_sem)
        right_load.start()
        loads = pltpu.make_async_copy(jac_hbm, jac_low, jac_sem)
        loads.start()

        lane = lax.broadcasted_iota(jnp.int32, full, 1)
        sub = lax.broadcasted_iota(jnp.int32, full, 0)

        def values(turn):
            return right_ref if turn == 0 else basis.at[turn - 1]

        def packed_with(packed, first, found):
            for at, value in enumerate(found, first):
                packed = jnp.where(lane // 2 == at, pltpu.roll(value, 2 * at + 1, 1), packed)
            return packed

        def remote(source, target, kind, turn, plane, device):
            return pltpu.make_async_remote_copy(
                src_ref=source,
                dst_ref=target,
                send_sem=send_sem.at[min(kind, KINDS)],
                recv_sem=recv_sem.at[turn % 2, plane, kind],
                device_id=device,
                device_id_type=MESH,
            )

        def send_edges(turn):
            for dz in (1, -1, 0):
                side_z = 0 if dz == 1 else 1

                def layer():
                    for plane in reversed(range(planes)):
                        for dy in (1, -1, 0):
                            device = beside(plane_steps[plane], dy, dz)
                            edge = pl.ds(rows - 1 if dy == 1 else 0, 1)
                            place = pl.ds(0 if dy == 1 else rows - 1, 1)
                            if dy == 0 and dz == 0:
                                continue
                            if dz == 0:
                                source, target, kind = values(turn).at[:, edge], halo_rows.at[turn, plane, :, place], 0
                            elif dy == 0:
                                source, target, kind = packs.at[turn], halo_cols.at[turn, plane, side_z], 1 + side_z
                            else:
                                source, target = packs.at[turn, edge], halo_corner.at[turn, plane, side_z, place]
                                kind = 3 + side_z
                            remote(source, target, kind, turn, plane, device).start()

                in_layer(dz, layer)

        def send_far(turn, group):
            for plane in range(1, planes):
                remote(
                    values(turn).at[pl.ds(group * span, span)], far_plane.at[turn, plane - 1, pl.ds(group * span, span)],
                    KINDS + group, turn, plane, beside(plane_steps[plane], 0, 0),
                ).start()

        def wait_edges(turn, plane):
            here = beside(1, 0, 0)
            both = halo_rows.at[turn, plane, :, pl.ds(0, 2)]
            remote(both, both, 0, turn, plane, here).wait_recv()
            for side_z, dz in ((0, -1), (1, 1)):

                def layer():
                    column = halo_cols.at[turn, plane, side_z]
                    remote(column, column, 1 + side_z, turn, plane, here).wait_recv()
                    corner = halo_corner.at[turn, plane, side_z, pl.ds(0, 2)]
                    remote(corner, corner, 3 + side_z, turn, plane, here).wait_recv()

                in_layer(dz, layer)

        def wait_far(turn, group, plane):
            whole = far_plane.at[turn, plane - 1, pl.ds(group * span, span)]
            remote(whole, whole, KINDS + group, turn, plane, beside(1, 0, 0)).wait_recv()

        def turned(value, way):
            if way == 0:
                return value
            return pltpu.roll(value, 1 if way < 0 else rows - 1, 0)

        side = {-1: sub == 0, 1: sub == rows - 1}

        def edge_columns(turn, plane):
            def edges(halo):
                low = jnp.where(below, halo[turn, plane, 0], 0.0)
                high = jnp.where(above, halo[turn, plane, 1], 0.0)
                return jnp.where(lane % 2 == 0, low, high)

            inner, outer = edges(halo_cols), edges(halo_corner)
            columns = {dy: jnp.where(side[dy], outer, turned(inner, dy)) for dy in (-1, 1)}
            columns[0] = inner
            return columns

        def stencil(turn, group, plane, columns, totals):
            for source in range(comp):
                for dy in (0, -1, 1):
                    along = {}
                    for r in range(each):
                        at = group * span + r * comp + source
                        value = values(turn)[at] if plane == 0 else far_plane[turn, plane - 1, at]
                        if dy != 0:
                            value = jnp.where(side[dy], halo_rows[turn, plane, at], turned(value, dy))
                        edge = pltpu.roll(columns[dy], lanes - 2 * at - 1, 1)
                        along[r, 1] = value
                        along[r, 0] = jnp.where(lane == lanes - 1, edge, value)
                        along[r, 2] = jnp.where(lane == 0, edge, value)
                    for dz in (1, 0, 2):
                        near = (dy + 1) * 3 + dz
                        for a in range(comp):
                            block = jac[plane, near, a * comp + source]
                            for r in range(each):
                                found = block * along[r, dz]
                                key = (r * comp + a, dz)
                                totals[key] = totals[key] + found if key in totals else found
            return totals

        def joined(totals):
            return [
                totals[at, 1] + (pltpu.roll(totals[at, 0], 1, 1) + pltpu.roll(totals[at, 2], lanes - 1, 1))
                for at in range(span)
            ]

        def vector(index, c):
            if index < rhs:
                return right_ref[index * comp + c]
            return prods[index // rhs - 1, (index % rhs) * comp + c]

        def dots(mine):
            own = [vector(mine, c) for c in range(comp)]
            for other in range(0, mine + 1):
                total = own[0] * vector(other, 0)
                for c in range(1, comp):
                    total = total + own[c] * vector(other, c)
                slot = pair_slot[mine, other]
                sums[slot : slot + 1, :] = jnp.sum(total, axis=0, keepdims=True)

        for slot in range(len(pair_list), pair_pad):
            sums[slot : slot + 1, :] = jnp.zeros((1, lanes), jnp.float32)
        right_load.wait()
        packs[0] = packed_with(jnp.zeros(full, jnp.float32), 0, [right_ref[at] for at in range(fields)])
        pl.semaphore_wait(barrier, greeted)
        send_edges(0)
        for group in range(groups):
            send_far(0, group)
        loads.wait()

        def widen(line, carry):
            for dz, shift in enumerate((lanes - 1, 0, 1)):
                near = line * 3 + dz

                def block(step_x, entry):
                    found = jac_low[9 * step_x + near, entry].astype(jnp.float32)
                    return pltpu.roll(found, shift, 1) if shift else found

                for entry in range(comp * comp):
                    jac[0, near, entry] = block(1, entry)
                    if merged:
                        found = jac_low[near, entry].astype(jnp.float32) + jac_low[18 + near, entry].astype(jnp.float32)
                        jac[1, near, entry] = pltpu.roll(found, shift, 1) if shift else found
                    else:
                        jac[1, near, entry] = block(0, entry)
                        jac[2, near, entry] = block(2, entry)
            return carry

        lax.fori_loop(0, 3, widen, 0)

        for turn in range(ITERS):
            wait_edges(turn, 0)
            columns = edge_columns(turn, 0)
            for group in range(groups):
                for (at, dz), total in stencil(turn, group, 0, columns, {}).items():
                    partial[group, dz, at] = total
            columns = {}
            packed = jnp.zeros(full, jnp.float32)
            for group in range(groups):
                first = group * span
                totals = {(at, dz): partial[group, dz, at] for at in range(span) for dz in range(3)}
                for plane in range(1, planes):
                    if group == 0:
                        wait_edges(turn, plane)
                        columns[plane] = edge_columns(turn, plane)
                    wait_far(turn, group, plane)
                    totals = stencil(turn, group, plane, columns[plane], totals)
                found = joined(totals)
                for at in range(span):
                    prods[turn, first + at] = found[at]
                if turn < ITERS - 1:
                    found = [found[at] - SHIFT * values(turn)[first + at] for at in range(span)]
                    for at in range(span):
                        basis[turn, first + at] = found[at]
                    packed = packed_with(packed, first, found)
                    if group == groups - 1:
                        packs[turn + 1] = packed
                        send_edges(turn + 1)
                    send_far(turn + 1, group)
                else:
                    for r in range(group * each, (group + 1) * each):
                        dots(rhs * (turn + 1) + r)
            if turn < ITERS - 1:
                for r in range(rhs):
                    dots(rhs * (turn + 1) + r)

        part[...] = jnp.sum(jnp.transpose(sums[...]), axis=0, keepdims=True)
        def reduce_copy(towards, source, target):
            return pltpu.make_async_remote_copy(
                src_ref=source,
                dst_ref=target,
                send_sem=red_send,
                recv_sem=red_recv,
                device_id=towards,
                device_id_type=MESH,
            )

        if devices <= 64:
            offsets = sorted(
                itertools.product(range(count_x), range(count_y), range(count_z)),
                key=lambda at: (-min(at[1], count_y - at[1]), -at[0], at[2]),
            )
            for ox, oy, oz in offsets:
                if (ox, oy, oz) != (0, 0, 0):
                    towards = (
                        lax.rem(my_x + ox, count_x), lax.rem(my_y + oy, count_y), lax.rem(my_z + oz, count_z)
                    )
                    reduce_copy(towards, part, parts.at[me]).start()
        else:

            def begin(step, carry):
                reduce_copy(coords(lax.rem(me + step, devices)), part, parts.at[me]).start()
                return carry

            lax.fori_loop(1, devices, begin, 0)
        parts[me] = part[...]
        for kind in range(KINDS + 1):
            for plane in range(planes):

                def layer():
                    for turn in range(ITERS):
                        if kind == 0:
                            whole = halo_rows.at[turn, plane, :, pl.ds(0, 2)]
                        elif kind < 3:
                            whole = halo_cols.at[turn, plane, kind - 1]
                        elif kind < 5:
                            whole = halo_corner.at[turn, plane, kind - 3, pl.ds(0, 2)]
                        elif plane > 0:
                            whole = far_plane.at[turn, plane - 1]
                        else:
                            continue
                        remote(whole, whole, kind, turn, plane, beside(1, 0, 0)).wait_send()

                in_layer((0, 1, -1, 1, -1, 0)[kind], layer)
        others = parts.at[pl.ds(0, devices - 1)]
        all_others = reduce_copy(beside(1, 0, 0), others, others)
        all_others.wait_recv()
        all_others.wait_send()
        found_parts = parts[...]
        count = devices
        while count > 1:
            half = count // 2
            rest = found_parts[2 * half :]
            found_parts = found_parts[:half] + found_parts[half : 2 * half]
            if count % 2:
                found_parts = jnp.concatenate([found_parts, rest], axis=0)
            count = count - half
        total_row = jnp.broadcast_to(found_parts[0], (rows, pair_pad))

        def entry(mine, other):
            slot = pair_slot[max(mine, other), min(mine, other)]
            return jnp.broadcast_to(total_row[:, slot : slot + 1], (rows, lanes))

        size = rhs * ITERS
        matrix = {}
        target = {}
        for i in range(size):
            for j in range(i + 1):
                matrix[i, j] = entry(rhs + i, rhs + j)
            for r in range(rhs):
                target[i, r] = entry(rhs + i, r)
        inverse = {}
        for k in range(size):
            inverse[k] = 1.0 / matrix[k, k]
            for i in range(k + 1, size):
                ratio = matrix[i, k] * inverse[k]
                for j in range(k + 1, i + 1):
                    matrix[i, j] = matrix[i, j] - ratio * matrix[j, k]
                for r in range(rhs):
                    target[i, r] = target[i, r] - ratio * target[k, r]
        weights = {}
        for k in range(size - 1, -1, -1):
            for r in range(rhs):
                weights[k, r] = target[k, r] * inverse[k]
                for prior in range(k):
                    target[prior, r] = target[prior, r] - matrix[k, prior] * weights[k, r]
        for c in range(comp):
            found = {}
            left = {r: right_ref[r * comp + c] for r in range(rhs)}
            for j in range(size - 1, -1, -1):
                direction = values(j // rhs)[(j % rhs) * comp + c]
                product = prods[j // rhs, (j % rhs) * comp + c]
                for r in range(rhs):
                    term = weights[j, r] * direction
                    found[r] = found[r] + term if r in found else term
                    left[r] = left[r] - weights[j, r] * product
            for r in range(rhs):
                sol_ref[r * comp + c] = found[r]
                res_ref[r * comp + c] = left[r]

    copies = (ITERS, planes)
    scratch = [
        pltpu.VMEM((fields,) + full, jnp.float32),
        pltpu.VMEM((ITERS - 1, fields) + full, jnp.float32),
        pltpu.VMEM((ITERS, fields) + full, jnp.float32),
        pltpu.VMEM((groups, 3, span) + full, jnp.float32),
        pltpu.VMEM((27, comp * comp) + full, jnp.bfloat16),
        pltpu.VMEM((planes, 9, comp * comp) + full, jnp.float32),
        pltpu.VMEM((ITERS,) + full, jnp.float32),
        pltpu.VMEM((ITERS, planes - 1, fields) + full, jnp.float32),
        pltpu.VMEM(copies + (fields,) + full, jnp.float32),
        pltpu.VMEM(copies + (2,) + full, jnp.float32),
        pltpu.VMEM(copies + (2,) + full, jnp.float32),
        pltpu.VMEM((pair_pad, lanes), jnp.float32),
        pltpu.VMEM((1, pair_pad), jnp.float32),
        pltpu.VMEM((devices, 1, pair_pad), jnp.float32),
        pltpu.SemaphoreType.DMA,
        pltpu.SemaphoreType.DMA,
        pltpu.SemaphoreType.DMA((KINDS + 1,)),
        pltpu.SemaphoreType.DMA((2, planes, KINDS + groups)),
        pltpu.SemaphoreType.DMA,
        pltpu.SemaphoreType.DMA,
    ]
    return kernel, scratch


def hand_over(found_ref, left_ref, sol_ref, res_ref, sem):
    copies = [
        pltpu.make_async_copy(found_ref, sol_ref, sem.at[0]),
        pltpu.make_async_copy(left_ref, res_ref, sem.at[1]),
    ]
    for copy in copies:
        copy.start()
    for copy in copies:
        copy.wait()


def shards(sizes, right_side, jacobian):
    rhs, comp, extent_x, rows, lanes = right_side.shape
    assert extent_x == 1
    kernel, scratch = make_kernel(sizes, rhs, comp, rows, lanes)
    shape = (rhs * comp, rows, lanes)
    vmem = pl.BlockSpec(memory_space=pltpu.VMEM)
    hbm = pl.BlockSpec(memory_space=pltpu.HBM)
    found, left = pl.pallas_call(
        kernel,
        out_shape=(pltpu.VMEM(shape, jnp.float32),) * 2,
        in_specs=[hbm, hbm],
        out_specs=(vmem, vmem),
        scratch_shapes=scratch,
        compiler_params=pltpu.CompilerParams(collective_id=0, has_side_effects=True),
    )(
        right_side.reshape(shape),
        jacobian.reshape(27, comp * comp, rows, lanes),
    )
    found, left = pl.pallas_call(
        hand_over,
        out_shape=(jax.ShapeDtypeStruct(shape, jnp.float32),) * 2,
        in_specs=[vmem, vmem],
        out_specs=(hbm, hbm),
        scratch_shapes=[pltpu.SemaphoreType.DMA((2,))],
        compiler_params=pltpu.CompilerParams(vmem_limit_bytes=24 * 2**20),
    )(found, left)
    return found.reshape(right_side.shape), left.reshape(right_side.shape)


def solution(mesh):
    sizes = tuple(mesh.shape[axis] for axis in AXES)
    in_specs = (P(None, None, *AXES), P(None, None, None, *AXES))
    out_specs = (P(None, None, *AXES), P(None, None, *AXES))
    return jax.shard_map(
        functools.partial(shards, sizes), mesh=mesh, in_specs=in_specs, out_specs=out_specs, check_vma=False
    )
```

```python
import functools
import itertools

import jax
import jax.numpy as jnp
from jax import lax
from jax.experimental import pallas as pl
from jax.experimental.pallas import tpu as pltpu
from jax.sharding import PartitionSpec as P

ITERS = 3
SHIFT = 9.0
MESH = pl.DeviceIdType.MESH
AXES = ("gx", "gy", "gz")
PAIRS = (2, 2)
PIECES = (2, 1, 1)
EARLY = 2
KINDS = 5


def parted(sizes, total):
    if sum(sizes) != total:
        sizes = (1,) * total
    ends = list(itertools.accumulate(sizes))
    return [range(end - size, end) for end, size in zip(ends, sizes)]


def make_kernel(sizes, rhs, comp, rows, lanes):
    count_x, count_y, count_z = sizes
    devices = count_x * count_y * count_z
    fields = rhs * comp
    merged = count_x == 2
    near_only = max(count_x // 2, count_y // 2, count_z - 1) <= ITERS
    plane_steps = (0, 1) if merged else (0, 1, -1)
    planes = len(plane_steps)
    near = parted(PAIRS, rhs)
    away = parted(PIECES, rhs)
    pair_list = []
    for mine in range(rhs, rhs * (ITERS + 1)):
        for other in range(0, mine + 1):
            pair_list.append((mine, other))
    pair_slot = {pair: slot for slot, pair in enumerate(pair_list)}
    pair_pad = -(-len(pair_list) // 128) * 128
    full = (rows, lanes)

    def kernel(
        right_hbm, jac_hbm, sol_ref, res_ref,
        right_ref, basis, prods, partial, jac_low, jac, packs,
        far_plane, halo_rows, halo_cols, halo_corner, sums, part, parts,
        right_sem, jac_sem, send_sem, recv_sem, red_send, red_recv,
    ):
        my_x, my_y, my_z = (lax.axis_index(axis) for axis in AXES)
        me = (my_x * count_y + my_y) * count_z + my_z

        def coords(index):
            return (index // (count_y * count_z), index // count_z % count_y, index % count_z)

        def beside(step_x, dy, dz):
            return (
                lax.rem(my_x + step_x + count_x, count_x),
                lax.rem(my_y + dy + count_y, count_y),
                jnp.clip(my_z + dz, 0, count_z - 1),
            )

        above = my_z < count_z - 1
        below = my_z > 0

        def in_layer(dz, act):
            if dz == 0:
                act()
            else:
                pl.when(above if dz == 1 else below)(act)

        barrier = pltpu.get_barrier_semaphore()

        def salute(device):
            pl.semaphore_signal(barrier, inc=1, device_id=device, device_id_type=MESH)

        if near_only:
            for dz in (1, -1, 0):
                def greet_layer():
                    for step_x, dy in itertools.product(reversed(plane_steps), (1, -1, 0)):
                        if (step_x, dy, dz) != (0, 0, 0):
                            salute(beside(step_x, dy, dz))

                in_layer(dz, greet_layer)
            greeted = planes * 3 * (1 + above.astype(jnp.int32) + below.astype(jnp.int32)) - 1
        else:

            def greet(step, carry):
                salute(coords(lax.rem(me + step, devices)))
                return carry

            lax.fori_loop(1, devices, greet, 0)
            greeted = devices - 1

        right_load = pltpu.make_async_copy(right_hbm, right_ref, right_sem)
        right_load.start()
        loads = pltpu.make_async_copy(jac_hbm, jac_low, jac_sem)
        loads.start()

        lane = lax.broadcasted_iota(jnp.int32, full, 1)
        sub = lax.broadcasted_iota(jnp.int32, full, 0)

        def values(turn):
            return right_ref if turn == 0 else basis.at[turn - 1]

        def packed_with(packed, first, found):
            for at, value in enumerate(found, first):
                packed = jnp.where(lane // 2 == at, pltpu.roll(value, 2 * at + 1, 1), packed)
            return packed

        def remote(source, target, kind, turn, plane, device):
            return pltpu.make_async_remote_copy(
                src_ref=source,
                dst_ref=target,
                send_sem=send_sem.at[min(kind, KINDS)],
                recv_sem=recv_sem.at[turn % 2, plane, kind],
                device_id=device,
                device_id_type=MESH,
            )

        def send_edges(turn):
            for dz in (1, -1, 0):
                side_z = 0 if dz == 1 else 1

                def layer():
                    for plane in reversed(range(planes)):
                        for dy in (1, -1, 0):
                            device = beside(plane_steps[plane], dy, dz)
                            edge = pl.ds(rows - 1 if dy == 1 else 0, 1)
                            place = pl.ds(0 if dy == 1 else rows - 1, 1)
                            if dy == 0 and dz == 0:
                                continue
                            if dz == 0:
                                source, target, kind = values(turn).at[:, edge], halo_rows.at[turn, plane, :, place], 0
                            elif dy == 0:
                                source, target, kind = packs.at[turn], halo_cols.at[turn, plane, side_z], 1 + side_z
                            else:
                                source, target = packs.at[turn, edge], halo_corner.at[turn, plane, side_z, place]
                                kind = 3 + side_z
                            remote(source, target, kind, turn, plane, device).start()

                in_layer(dz, layer)

        def piece(index):
            return pl.ds(away[index].start * comp, len(away[index]) * comp)

        def send_far(turn, index):
            for plane in range(1, planes):
                remote(
                    values(turn).at[piece(index)], far_plane.at[turn, plane - 1, piece(index)],
                    KINDS + index, turn, plane, beside(plane_steps[plane], 0, 0),
                ).start()

        def wait_edges(turn, plane):
            here = beside(1, 0, 0)
            both = halo_rows.at[turn, plane, :, pl.ds(0, 2)]
            remote(both, both, 0, turn, plane, here).wait_recv()
            for side_z, dz in ((0, -1), (1, 1)):

                def layer():
                    column = halo_cols.at[turn, plane, side_z]
                    remote(column, column, 1 + side_z, turn, plane, here).wait_recv()
                    corner = halo_corner.at[turn, plane, side_z, pl.ds(0, 2)]
                    remote(corner, corner, 3 + side_z, turn, plane, here).wait_recv()

                in_layer(dz, layer)

        def wait_far(turn, index, plane):
            whole = far_plane.at[turn, plane - 1, piece(index)]
            remote(whole, whole, KINDS + index, turn, plane, beside(1, 0, 0)).wait_recv()

        def turned(value, way):
            if way == 0:
                return value
            return pltpu.roll(value, 1 if way < 0 else rows - 1, 0)

        side = {-1: sub == 0, 1: sub == rows - 1}

        def edge_columns(turn, plane):
            def edges(halo):
                low = jnp.where(below, halo[turn, plane, 0], 0.0)
                high = jnp.where(above, halo[turn, plane, 1], 0.0)
                return jnp.where(lane % 2 == 0, low, high)

            inner, outer = edges(halo_cols), edges(halo_corner)
            columns = {dy: jnp.where(side[dy], outer, turned(inner, dy)) for dy in (-1, 1)}
            columns[0] = inner
            return columns

        def stencil(turn, chosen, plane, columns, totals):
            for source in range(comp):
                for dy in (0, -1, 1):
                    along = {}
                    for r in chosen:
                        at = r * comp + source
                        value = values(turn)[at] if plane == 0 else far_plane[turn, plane - 1, at]
                        if dy != 0:
                            value = jnp.where(side[dy], halo_rows[turn, plane, at], turned(value, dy))
                        edge = pltpu.roll(columns[dy], lanes - 2 * at - 1, 1)
                        along[r, 1] = value
                        along[r, 0] = jnp.where(lane == lanes - 1, edge, value)
                        along[r, 2] = jnp.where(lane == 0, edge, value)
                    for dz in (1, 0, 2):
                        spot = (dy + 1) * 3 + dz
                        for a in range(comp):
                            block = jac[plane, spot, a * comp + source]
                            for r in chosen:
                                found = block * along[r, dz]
                                key = (r * comp + a, dz)
                                totals[key] = totals[key] + found if key in totals else found
            return totals

        def joined(totals, at):
            return totals[at, 1] + (pltpu.roll(totals[at, 0], 1, 1) + pltpu.roll(totals[at, 2], lanes - 1, 1))

        def vector(index, c):
            if index < rhs:
                return right_ref[index * comp + c]
            return prods[index // rhs - 1, (index % rhs) * comp + c]

        def dots(mine):
            own = [vector(mine, c) for c in range(comp)]
            for other in range(0, mine + 1):
                total = own[0] * vector(other, 0)
                for c in range(1, comp):
                    total = total + own[c] * vector(other, c)
                slot = pair_slot[mine, other]
                sums[slot : slot + 1, :] = jnp.sum(total, axis=0, keepdims=True)

        for slot in range(len(pair_list), pair_pad):
            sums[slot : slot + 1, :] = jnp.zeros((1, lanes), jnp.float32)
        right_load.wait()
        packs[0] = packed_with(jnp.zeros(full, jnp.float32), 0, [right_ref[at] for at in range(fields)])
        pl.semaphore_wait(barrier, greeted)
        send_edges(0)
        for index in range(len(away)):
            send_far(0, index)
        loads.wait()

        def widen(line, carry):
            for dz, shift in enumerate((lanes - 1, 0, 1)):
                near = line * 3 + dz

                def block(step_x, entry):
                    found = jac_low[9 * step_x + near, entry].astype(jnp.float32)
                    return pltpu.roll(found, shift, 1) if shift else found

                for entry in range(comp * comp):
                    jac[0, near, entry] = block(1, entry)
                    if merged:
                        found = jac_low[near, entry].astype(jnp.float32) + jac_low[18 + near, entry].astype(jnp.float32)
                        jac[1, near, entry] = pltpu.roll(found, shift, 1) if shift else found
                    else:
                        jac[1, near, entry] = block(0, entry)
                        jac[2, near, entry] = block(2, entry)
            return carry

        lax.fori_loop(0, 3, widen, 0)

        for turn in range(ITERS):
            wait_edges(turn, 0)
            columns = edge_columns(turn, 0)
            for chosen in near:
                for (at, dz), total in stencil(turn, chosen, 0, columns, {}).items():
                    partial[dz, at] = total
            columns = {}
            packed = jnp.zeros(full, jnp.float32)
            for index, chosen in enumerate(away):
                span = range(chosen.start * comp, chosen.stop * comp)
                totals = {(at, dz): partial[dz, at] for at in span for dz in range(3)}
                for plane in range(1, planes):
                    if index == 0:
                        wait_edges(turn, plane)
                        columns[plane] = edge_columns(turn, plane)
                    wait_far(turn, index, plane)
                    totals = stencil(turn, chosen, plane, columns[plane], totals)
                found = [joined(totals, at) for at in span]
                for at, value in zip(span, found):
                    prods[turn, at] = value
                if turn == ITERS - 1:
                    for r in chosen:
                        dots(rhs * (turn + 1) + r)
                    continue
                found = [value - SHIFT * values(turn)[at] for at, value in zip(span, found)]
                for at, value in zip(span, found):
                    basis[turn, at] = value
                packed = packed_with(packed, span.start, found)
                if index < EARLY:
                    send_far(turn + 1, index)
                if index == len(away) - 1:
                    packs[turn + 1] = packed
                    send_edges(turn + 1)
                    for later in range(EARLY, len(away)):
                        send_far(turn + 1, later)
            if turn < ITERS - 1:
                for r in range(rhs):
                    dots(rhs * (turn + 1) + r)

        part[...] = jnp.sum(jnp.transpose(sums[...]), axis=0, keepdims=True)
        def reduce_copy(towards, source, target):
            return pltpu.make_async_remote_copy(
                src_ref=source,
                dst_ref=target,
                send_sem=red_send,
                recv_sem=red_recv,
                device_id=towards,
                device_id_type=MESH,
            )

        if devices <= 64:
            offsets = sorted(
                itertools.product(range(count_x), range(count_y), range(count_z)),
                key=lambda at: (-min(at[1], count_y - at[1]), -at[0], at[2]),
            )
            for ox, oy, oz in offsets:
                if (ox, oy, oz) != (0, 0, 0):
                    towards = (
                        lax.rem(my_x + ox, count_x), lax.rem(my_y + oy, count_y), lax.rem(my_z + oz, count_z)
                    )
                    reduce_copy(towards, part, parts.at[me]).start()
        else:

            def begin(step, carry):
                reduce_copy(coords(lax.rem(me + step, devices)), part, parts.at[me]).start()
                return carry

            lax.fori_loop(1, devices, begin, 0)
        parts[me] = part[...]
        for kind in range(KINDS + 1):
            for plane in range(planes):

                def layer():
                    for turn in range(ITERS):
                        if kind == 0:
                            whole = halo_rows.at[turn, plane, :, pl.ds(0, 2)]
                        elif kind < 3:
                            whole = halo_cols.at[turn, plane, kind - 1]
                        elif kind < 5:
                            whole = halo_corner.at[turn, plane, kind - 3, pl.ds(0, 2)]
                        elif plane > 0:
                            whole = far_plane.at[turn, plane - 1]
                        else:
                            continue
                        remote(whole, whole, kind, turn, plane, beside(1, 0, 0)).wait_send()

                in_layer((0, 1, -1, 1, -1, 0)[kind], layer)
        others = parts.at[pl.ds(0, devices - 1)]
        all_others = reduce_copy(beside(1, 0, 0), others, others)
        all_others.wait_recv()
        all_others.wait_send()
        found_parts = parts[...]
        count = devices
        while count > 1:
            half = count // 2
            rest = found_parts[2 * half :]
            found_parts = found_parts[:half] + found_parts[half : 2 * half]
            if count % 2:
                found_parts = jnp.concatenate([found_parts, rest], axis=0)
            count = count - half
        total_row = jnp.broadcast_to(found_parts[0], (rows, pair_pad))

        def entry(mine, other):
            slot = pair_slot[max(mine, other), min(mine, other)]
            return jnp.broadcast_to(total_row[:, slot : slot + 1], (rows, lanes))

        size = rhs * ITERS
        matrix = {}
        target = {}
        for i in range(size):
            for j in range(i + 1):
                matrix[i, j] = entry(rhs + i, rhs + j)
            for r in range(rhs):
                target[i, r] = entry(rhs + i, r)
        inverse = {}
        for k in range(size):
            inverse[k] = 1.0 / matrix[k, k]
            for i in range(k + 1, size):
                ratio = matrix[i, k] * inverse[k]
                for j in range(k + 1, i + 1):
                    matrix[i, j] = matrix[i, j] - ratio * matrix[j, k]
                for r in range(rhs):
                    target[i, r] = target[i, r] - ratio * target[k, r]
        weights = {}
        for k in range(size - 1, -1, -1):
            for r in range(rhs):
                weights[k, r] = target[k, r] * inverse[k]
                for prior in range(k):
                    target[prior, r] = target[prior, r] - matrix[k, prior] * weights[k, r]
        for c in range(comp):
            found = {}
            left = {r: right_ref[r * comp + c] for r in range(rhs)}
            for j in range(size - 1, -1, -1):
                direction = values(j // rhs)[(j % rhs) * comp + c]
                product = prods[j // rhs, (j % rhs) * comp + c]
                for r in range(rhs):
                    term = weights[j, r] * direction
                    found[r] = found[r] + term if r in found else term
                    left[r] = left[r] - weights[j, r] * product
            for r in range(rhs):
                sol_ref[r * comp + c] = found[r]
                res_ref[r * comp + c] = left[r]

    copies = (ITERS, planes)
    scratch = [
        pltpu.VMEM((fields,) + full, jnp.float32),
        pltpu.VMEM((ITERS - 1, fields) + full, jnp.float32),
        pltpu.VMEM((ITERS, fields) + full, jnp.float32),
        pltpu.VMEM((3, fields) + full, jnp.float32),
        pltpu.VMEM((27, comp * comp) + full, jnp.bfloat16),
        pltpu.VMEM((planes, 9, comp * comp) + full, jnp.float32),
        pltpu.VMEM((ITERS,) + full, jnp.float32),
        pltpu.VMEM((ITERS, planes - 1, fields) + full, jnp.float32),
        pltpu.VMEM(copies + (fields,) + full, jnp.float32),
        pltpu.VMEM(copies + (2,) + full, jnp.float32),
        pltpu.VMEM(copies + (2,) + full, jnp.float32),
        pltpu.VMEM((pair_pad, lanes), jnp.float32),
        pltpu.VMEM((1, pair_pad), jnp.float32),
        pltpu.VMEM((devices, 1, pair_pad), jnp.float32),
        pltpu.SemaphoreType.DMA,
        pltpu.SemaphoreType.DMA,
        pltpu.SemaphoreType.DMA((KINDS + 1,)),
        pltpu.SemaphoreType.DMA((2, planes, KINDS + len(away))),
        pltpu.SemaphoreType.DMA,
        pltpu.SemaphoreType.DMA,
    ]
    return kernel, scratch


def hand_over(found_ref, left_ref, sol_ref, res_ref, sem):
    copies = [
        pltpu.make_async_copy(found_ref, sol_ref, sem.at[0]),
        pltpu.make_async_copy(left_ref, res_ref, sem.at[1]),
    ]
    for copy in copies:
        copy.start()
    for copy in copies:
        copy.wait()


def shards(sizes, right_side, jacobian):
    rhs, comp, extent_x, rows, lanes = right_side.shape
    assert extent_x == 1
    kernel, scratch = make_kernel(sizes, rhs, comp, rows, lanes)
    shape = (rhs * comp, rows, lanes)
    vmem = pl.BlockSpec(memory_space=pltpu.VMEM)
    hbm = pl.BlockSpec(memory_space=pltpu.HBM)
    found, left = pl.pallas_call(
        kernel,
        out_shape=(pltpu.VMEM(shape, jnp.float32),) * 2,
        in_specs=[hbm, hbm],
        out_specs=(vmem, vmem),
        scratch_shapes=scratch,
        compiler_params=pltpu.CompilerParams(collective_id=0, has_side_effects=True),
    )(
        right_side.reshape(shape),
        jacobian.reshape(27, comp * comp, rows, lanes),
    )
    found, left = pl.pallas_call(
        hand_over,
        out_shape=(jax.ShapeDtypeStruct(shape, jnp.float32),) * 2,
        in_specs=[vmem, vmem],
        out_specs=(hbm, hbm),
        scratch_shapes=[pltpu.SemaphoreType.DMA((2,))],
        compiler_params=pltpu.CompilerParams(vmem_limit_bytes=24 * 2**20),
    )(found, left)
    return found.reshape(right_side.shape), left.reshape(right_side.shape)


def solution(mesh):
    sizes = tuple(mesh.shape[axis] for axis in AXES)
    in_specs = (P(None, None, *AXES), P(None, None, None, *AXES))
    out_specs = (P(None, None, *AXES), P(None, None, *AXES))
    return jax.shard_map(
        functools.partial(shards, sizes), mesh=mesh, in_specs=in_specs, out_specs=out_specs, check_vma=False
    )
```

```python
import functools
import itertools

import jax
import jax.numpy as jnp
from jax import lax
from jax.experimental import pallas as pl
from jax.experimental.pallas import tpu as pltpu
from jax.sharding import PartitionSpec as P

ITERS = 3
SHIFT = 9.0
MESH = pl.DeviceIdType.MESH
AXES = ("gx", "gy", "gz")
PAIRS = (2, 2)
PIECES = (2, 1, 1)
EARLY = 1
KINDS = 5


def parted(sizes, total):
    if sum(sizes) != total:
        sizes = (1,) * total
    ends = list(itertools.accumulate(sizes))
    return [range(end - size, end) for end, size in zip(ends, sizes)]


def make_kernel(sizes, rhs, comp, rows, lanes):
    count_x, count_y, count_z = sizes
    devices = count_x * count_y * count_z
    fields = rhs * comp
    merged = count_x == 2
    near_only = max(count_x // 2, count_y // 2, count_z - 1) <= ITERS
    plane_steps = (0, 1) if merged else (0, 1, -1)
    planes = len(plane_steps)
    near = parted(PAIRS, rhs)
    away = parted(PIECES, rhs)
    pair_list = []
    for mine in range(rhs, rhs * (ITERS + 1)):
        for other in range(0, mine + 1):
            pair_list.append((mine, other))
    pair_slot = {pair: slot for slot, pair in enumerate(pair_list)}
    pair_pad = -(-len(pair_list) // 128) * 128
    full = (rows, lanes)

    def kernel(
        right_hbm, jac_hbm, sol_ref, res_ref,
        right_ref, basis, prods, partial, jac_low, jac, packs,
        far_plane, halo_rows, halo_cols, halo_corner, sums, part, parts,
        right_sem, jac_sem, send_sem, recv_sem, red_send, red_recv,
    ):
        my_x, my_y, my_z = (lax.axis_index(axis) for axis in AXES)
        me = (my_x * count_y + my_y) * count_z + my_z

        def coords(index):
            return (index // (count_y * count_z), index // count_z % count_y, index % count_z)

        def beside(step_x, dy, dz):
            return (
                lax.rem(my_x + step_x + count_x, count_x),
                lax.rem(my_y + dy + count_y, count_y),
                jnp.clip(my_z + dz, 0, count_z - 1),
            )

        above = my_z < count_z - 1
        below = my_z > 0

        def in_layer(dz, act):
            if dz == 0:
                act()
            else:
                pl.when(above if dz == 1 else below)(act)

        barrier = pltpu.get_barrier_semaphore()

        def salute(device):
            pl.semaphore_signal(barrier, inc=1, device_id=device, device_id_type=MESH)

        if near_only:
            for dz in (1, -1, 0):
                def greet_layer():
                    for step_x, dy in itertools.product(reversed(plane_steps), (1, -1, 0)):
                        if (step_x, dy, dz) != (0, 0, 0):
                            salute(beside(step_x, dy, dz))

                in_layer(dz, greet_layer)
            greeted = planes * 3 * (1 + above.astype(jnp.int32) + below.astype(jnp.int32)) - 1
        else:

            def greet(step, carry):
                salute(coords(lax.rem(me + step, devices)))
                return carry

            lax.fori_loop(1, devices, greet, 0)
            greeted = devices - 1

        right_load = pltpu.make_async_copy(right_hbm, right_ref, right_sem)
        right_load.start()
        loads = pltpu.make_async_copy(jac_hbm, jac_low, jac_sem)
        loads.start()

        lane = lax.broadcasted_iota(jnp.int32, full, 1)
        sub = lax.broadcasted_iota(jnp.int32, full, 0)

        def values(turn):
            return right_ref if turn == 0 else basis.at[turn - 1]

        def packed_with(packed, first, found):
            for at, value in enumerate(found, first):
                packed = jnp.where(lane // 2 == at, pltpu.roll(value, 2 * at + 1, 1), packed)
            return packed

        def remote(source, target, kind, turn, plane, device):
            return pltpu.make_async_remote_copy(
                src_ref=source,
                dst_ref=target,
                send_sem=send_sem.at[min(kind, KINDS)],
                recv_sem=recv_sem.at[turn % 2, plane, kind],
                device_id=device,
                device_id_type=MESH,
            )

        def send_edges(turn):
            for dz in (1, -1, 0):
                side_z = 0 if dz == 1 else 1

                def layer():
                    for plane in reversed(range(planes)):
                        for dy in (1, -1, 0):
                            device = beside(plane_steps[plane], dy, dz)
                            edge = pl.ds(rows - 1 if dy == 1 else 0, 1)
                            place = pl.ds(0 if dy == 1 else rows - 1, 1)
                            if dy == 0 and dz == 0:
                                continue
                            if dz == 0:
                                source, target, kind = values(turn).at[:, edge], halo_rows.at[turn, plane, :, place], 0
                            elif dy == 0:
                                source, target, kind = packs.at[turn], halo_cols.at[turn, plane, side_z], 1 + side_z
                            else:
                                source, target = packs.at[turn, edge], halo_corner.at[turn, plane, side_z, place]
                                kind = 3 + side_z
                            remote(source, target, kind, turn, plane, device).start()

                in_layer(dz, layer)

        def piece(index):
            return pl.ds(away[index].start * comp, len(away[index]) * comp)

        def send_far(turn, index):
            for plane in range(1, planes):
                remote(
                    values(turn).at[piece(index)], far_plane.at[turn, plane - 1, piece(index)],
                    KINDS + index, turn, plane, beside(plane_steps[plane], 0, 0),
                ).start()

        def wait_edges(turn, plane):
            here = beside(1, 0, 0)
            both = halo_rows.at[turn, plane, :, pl.ds(0, 2)]
            remote(both, both, 0, turn, plane, here).wait_recv()
            for side_z, dz in ((0, -1), (1, 1)):

                def layer():
                    column = halo_cols.at[turn, plane, side_z]
                    remote(column, column, 1 + side_z, turn, plane, here).wait_recv()
                    corner = halo_corner.at[turn, plane, side_z, pl.ds(0, 2)]
                    remote(corner, corner, 3 + side_z, turn, plane, here).wait_recv()

                in_layer(dz, layer)

        def wait_far(turn, index, plane):
            whole = far_plane.at[turn, plane - 1, piece(index)]
            remote(whole, whole, KINDS + index, turn, plane, beside(1, 0, 0)).wait_recv()

        def turned(value, way):
            if way == 0:
                return value
            return pltpu.roll(value, 1 if way < 0 else rows - 1, 0)

        side = {-1: sub == 0, 1: sub == rows - 1}

        def edge_columns(turn, plane):
            def edges(halo):
                low = jnp.where(below, halo[turn, plane, 0], 0.0)
                high = jnp.where(above, halo[turn, plane, 1], 0.0)
                return jnp.where(lane % 2 == 0, low, high)

            inner, outer = edges(halo_cols), edges(halo_corner)
            columns = {dy: jnp.where(side[dy], outer, turned(inner, dy)) for dy in (-1, 1)}
            columns[0] = inner
            return columns

        def stencil(turn, chosen, plane, columns, totals):
            for source in range(comp):
                for dy in (0, -1, 1):
                    along = {}
                    for r in chosen:
                        at = r * comp + source
                        value = values(turn)[at] if plane == 0 else far_plane[turn, plane - 1, at]
                        if dy != 0:
                            value = jnp.where(side[dy], halo_rows[turn, plane, at], turned(value, dy))
                        edge = pltpu.roll(columns[dy], lanes - 2 * at - 1, 1)
                        along[r, 1] = value
                        along[r, 0] = jnp.where(lane == lanes - 1, edge, value)
                        along[r, 2] = jnp.where(lane == 0, edge, value)
                    for dz in (1, 0, 2):
                        spot = (dy + 1) * 3 + dz
                        for a in range(comp):
                            block = jac[plane, spot, a * comp + source]
                            for r in chosen:
                                found = block * along[r, dz]
                                key = (r * comp + a, dz)
                                totals[key] = totals[key] + found if key in totals else found
            return totals

        def joined(totals, at):
            return totals[at, 1] + (pltpu.roll(totals[at, 0], 1, 1) + pltpu.roll(totals[at, 2], lanes - 1, 1))

        def vector(index, c):
            if index < rhs:
                return right_ref[index * comp + c]
            return prods[index // rhs - 1, (index % rhs) * comp + c]

        def dots(mine):
            own = [vector(mine, c) for c in range(comp)]
            for other in range(0, mine + 1):
                total = own[0] * vector(other, 0)
                for c in range(1, comp):
                    total = total + own[c] * vector(other, c)
                slot = pair_slot[mine, other]
                sums[slot : slot + 1, :] = jnp.sum(total, axis=0, keepdims=True)

        for slot in range(len(pair_list), pair_pad):
            sums[slot : slot + 1, :] = jnp.zeros((1, lanes), jnp.float32)
        right_load.wait()
        packs[0] = packed_with(jnp.zeros(full, jnp.float32), 0, [right_ref[at] for at in range(fields)])
        pl.semaphore_wait(barrier, greeted)
        send_edges(0)
        for index in range(len(away)):
            send_far(0, index)
        loads.wait()

        def widen(line, carry):
            for dz, shift in enumerate((lanes - 1, 0, 1)):
                near = line * 3 + dz

                def block(step_x, entry):
                    found = jac_low[9 * step_x + near, entry].astype(jnp.float32)
                    return pltpu.roll(found, shift, 1) if shift else found

                for entry in range(comp * comp):
                    jac[0, near, entry] = block(1, entry)
                    if merged:
                        found = jac_low[near, entry].astype(jnp.float32) + jac_low[18 + near, entry].astype(jnp.float32)
                        jac[1, near, entry] = pltpu.roll(found, shift, 1) if shift else found
                    else:
                        jac[1, near, entry] = block(0, entry)
                        jac[2, near, entry] = block(2, entry)
            return carry

        lax.fori_loop(0, 3, widen, 0)

        for turn in range(ITERS):
            wait_edges(turn, 0)
            columns = edge_columns(turn, 0)
            for chosen in near:
                for (at, dz), total in stencil(turn, chosen, 0, columns, {}).items():
                    partial[dz, at] = total
            columns = {}
            packed = jnp.zeros(full, jnp.float32)
            for index, chosen in enumerate(away):
                span = range(chosen.start * comp, chosen.stop * comp)
                totals = {(at, dz): partial[dz, at] for at in span for dz in range(3)}
                for plane in range(1, planes):
                    if index == 0:
                        wait_edges(turn, plane)
                        columns[plane] = edge_columns(turn, plane)
                    wait_far(turn, index, plane)
                    totals = stencil(turn, chosen, plane, columns[plane], totals)
                found = [joined(totals, at) for at in span]
                for at, value in zip(span, found):
                    prods[turn, at] = value
                if turn == ITERS - 1:
                    for r in chosen:
                        dots(rhs * (turn + 1) + r)
                    continue
                found = [value - SHIFT * values(turn)[at] for at, value in zip(span, found)]
                for at, value in zip(span, found):
                    basis[turn, at] = value
                packed = packed_with(packed, span.start, found)
                if index < EARLY:
                    send_far(turn + 1, index)
                if index == len(away) - 1:
                    packs[turn + 1] = packed
                    send_edges(turn + 1)
                    for later in range(EARLY, len(away)):
                        send_far(turn + 1, later)
            if turn < ITERS - 1:
                for r in range(rhs):
                    dots(rhs * (turn + 1) + r)

        part[...] = jnp.sum(jnp.transpose(sums[...]), axis=0, keepdims=True)
        def reduce_copy(towards, source, target):
            return pltpu.make_async_remote_copy(
                src_ref=source,
                dst_ref=target,
                send_sem=red_send,
                recv_sem=red_recv,
                device_id=towards,
                device_id_type=MESH,
            )

        if devices <= 64:
            offsets = sorted(
                itertools.product(range(count_x), range(count_y), range(count_z)),
                key=lambda at: (-min(at[1], count_y - at[1]), -at[0], at[2]),
            )
            for ox, oy, oz in offsets:
                if (ox, oy, oz) != (0, 0, 0):
                    towards = (
                        lax.rem(my_x + ox, count_x), lax.rem(my_y + oy, count_y), lax.rem(my_z + oz, count_z)
                    )
                    reduce_copy(towards, part, parts.at[me]).start()
        else:

            def begin(step, carry):
                reduce_copy(coords(lax.rem(me + step, devices)), part, parts.at[me]).start()
                return carry

            lax.fori_loop(1, devices, begin, 0)
        parts[me] = part[...]
        for kind in range(KINDS + 1):
            for plane in range(planes):

                def layer():
                    for turn in range(ITERS):
                        if kind == 0:
                            whole = halo_rows.at[turn, plane, :, pl.ds(0, 2)]
                        elif kind < 3:
                            whole = halo_cols.at[turn, plane, kind - 1]
                        elif kind < 5:
                            whole = halo_corner.at[turn, plane, kind - 3, pl.ds(0, 2)]
                        elif plane > 0:
                            whole = far_plane.at[turn, plane - 1]
                        else:
                            continue
                        remote(whole, whole, kind, turn, plane, beside(1, 0, 0)).wait_send()

                in_layer((0, 1, -1, 1, -1, 0)[kind], layer)
        others = parts.at[pl.ds(0, devices - 1)]
        all_others = reduce_copy(beside(1, 0, 0), others, others)
        all_others.wait_recv()
        all_others.wait_send()
        found_parts = parts[...]
        count = devices
        while count > 1:
            half = count // 2
            rest = found_parts[2 * half :]
            found_parts = found_parts[:half] + found_parts[half : 2 * half]
            if count % 2:
                found_parts = jnp.concatenate([found_parts, rest], axis=0)
            count = count - half
        total_row = jnp.broadcast_to(found_parts[0], (rows, pair_pad))

        def entry(mine, other):
            slot = pair_slot[max(mine, other), min(mine, other)]
            return jnp.broadcast_to(total_row[:, slot : slot + 1], (rows, lanes))

        size = rhs * ITERS
        matrix = {}
        target = {}
        for i in range(size):
            for j in range(i + 1):
                matrix[i, j] = entry(rhs + i, rhs + j)
            for r in range(rhs):
                target[i, r] = entry(rhs + i, r)
        inverse = {}
        for k in range(size):
            inverse[k] = 1.0 / matrix[k, k]
            for i in range(k + 1, size):
                ratio = matrix[i, k] * inverse[k]
                for j in range(k + 1, i + 1):
                    matrix[i, j] = matrix[i, j] - ratio * matrix[j, k]
                for r in range(rhs):
                    target[i, r] = target[i, r] - ratio * target[k, r]
        weights = {}
        for k in range(size - 1, -1, -1):
            for r in range(rhs):
                weights[k, r] = target[k, r] * inverse[k]
                for prior in range(k):
                    target[prior, r] = target[prior, r] - matrix[k, prior] * weights[k, r]
        for c in range(comp):
            found = {}
            left = {r: right_ref[r * comp + c] for r in range(rhs)}
            for j in range(size - 1, -1, -1):
                direction = values(j // rhs)[(j % rhs) * comp + c]
                product = prods[j // rhs, (j % rhs) * comp + c]
                for r in range(rhs):
                    term = weights[j, r] * direction
                    found[r] = found[r] + term if r in found else term
                    left[r] = left[r] - weights[j, r] * product
            for r in range(rhs):
                sol_ref[r * comp + c] = found[r]
                res_ref[r * comp + c] = left[r]

    copies = (ITERS, planes)
    scratch = [
        pltpu.VMEM((fields,) + full, jnp.float32),
        pltpu.VMEM((ITERS - 1, fields) + full, jnp.float32),
        pltpu.VMEM((ITERS, fields) + full, jnp.float32),
        pltpu.VMEM((3, fields) + full, jnp.float32),
        pltpu.VMEM((27, comp * comp) + full, jnp.bfloat16),
        pltpu.VMEM((planes, 9, comp * comp) + full, jnp.float32),
        pltpu.VMEM((ITERS,) + full, jnp.float32),
        pltpu.VMEM((ITERS, planes - 1, fields) + full, jnp.float32),
        pltpu.VMEM(copies + (fields,) + full, jnp.float32),
        pltpu.VMEM(copies + (2,) + full, jnp.float32),
        pltpu.VMEM(copies + (2,) + full, jnp.float32),
        pltpu.VMEM((pair_pad, lanes), jnp.float32),
        pltpu.VMEM((1, pair_pad), jnp.float32),
        pltpu.VMEM((devices, 1, pair_pad), jnp.float32),
        pltpu.SemaphoreType.DMA,
        pltpu.SemaphoreType.DMA,
        pltpu.SemaphoreType.DMA((KINDS + 1,)),
        pltpu.SemaphoreType.DMA((2, planes, KINDS + len(away))),
        pltpu.SemaphoreType.DMA,
        pltpu.SemaphoreType.DMA,
    ]
    return kernel, scratch


def hand_over(found_ref, left_ref, sol_ref, res_ref, sem):
    copies = [
        pltpu.make_async_copy(found_ref, sol_ref, sem.at[0]),
        pltpu.make_async_copy(left_ref, res_ref, sem.at[1]),
    ]
    for copy in copies:
        copy.start()
    for copy in copies:
        copy.wait()


def shards(sizes, right_side, jacobian):
    rhs, comp, extent_x, rows, lanes = right_side.shape
    assert extent_x == 1
    kernel, scratch = make_kernel(sizes, rhs, comp, rows, lanes)
    shape = (rhs * comp, rows, lanes)
    vmem = pl.BlockSpec(memory_space=pltpu.VMEM)
    hbm = pl.BlockSpec(memory_space=pltpu.HBM)
    found, left = pl.pallas_call(
        kernel,
        out_shape=(pltpu.VMEM(shape, jnp.float32),) * 2,
        in_specs=[hbm, hbm],
        out_specs=(vmem, vmem),
        scratch_shapes=scratch,
        compiler_params=pltpu.CompilerParams(collective_id=0, has_side_effects=True),
    )(
        right_side.reshape(shape),
        jacobian.reshape(27, comp * comp, rows, lanes),
    )
    found, left = pl.pallas_call(
        hand_over,
        out_shape=(jax.ShapeDtypeStruct(shape, jnp.float32),) * 2,
        in_specs=[vmem, vmem],
        out_specs=(hbm, hbm),
        scratch_shapes=[pltpu.SemaphoreType.DMA((2,))],
        compiler_params=pltpu.CompilerParams(vmem_limit_bytes=24 * 2**20),
    )(found, left)
    return found.reshape(right_side.shape), left.reshape(right_side.shape)


def solution(mesh):
    sizes = tuple(mesh.shape[axis] for axis in AXES)
    in_specs = (P(None, None, *AXES), P(None, None, None, *AXES))
    out_specs = (P(None, None, *AXES), P(None, None, *AXES))
    return jax.shard_map(
        functools.partial(shards, sizes), mesh=mesh, in_specs=in_specs, out_specs=out_specs, check_vma=False
    )
```
